8 devices in a mesh: batch: 2 (over z, y), dap: 4 (over x, core).
Axes of the slice: x: 2, y: 2, z: 1, core: 2. Of those that a mesh axis runs over, the one named last changes fastest.
Arguments:
- z_pair: bfloat16 [1024, 512, 128], P(('batch', 'dap')), parts along dimension 0
- pair_mask: int32 [1024, 512], P(('batch', 'dap')), parts along dimension 0
- dz_out: bfloat16 [1024, 512, 128], P(('batch', 'dap')), parts along dimension 0
- ln_in_scale: bfloat16 [128], replicated
- ln_in_offset: bfloat16 [128], replicated
- w_in: bfloat16 [128, 512], replicated
- b_in: bfloat16 [512], replicated
- ln_out_scale: bfloat16 [128], replicated
- ln_out_offset: bfloat16 [128], replicated
- w_out: bfloat16 [128, 128], replicated
- b_out: bfloat16 [128], replicated
- w_gate: bfloat16 [128, 128], replicated
- b_gate: bfloat16 [128], replicated
Outputs:
- output 1: bfloat16 [1024, 512, 128], P(('batch', 'dap')), parts along dimension 0
- output 2: bfloat16 [256], P('batch'), parts along dimension 0
- output 3: bfloat16 [256], P('batch'), parts along dimension 0
- output 4: bfloat16 [256, 512], P('batch'), parts along dimension 0
- output 5: bfloat16 [1024], P('batch'), parts along dimension 0
- output 6: bfloat16 [256], P('batch'), parts along dimension 0
- output 7: bfloat16 [256], P('batch'), parts along dimension 0
- output 8: bfloat16 [256, 128], P('batch'), parts along dimension 0
- output 9: bfloat16 [256], P('batch'), parts along dimension 0
- output 10: bfloat16 [256, 128], P('batch'), parts along dimension 0
- output 11: bfloat16 [256], P('batch'), parts along dimension 0
There are 2 independent parts. The reference program is written for one: setup_inputs(seed, part) draws one part's arguments, and reference() takes and returns one part's arrays. A program takes and returns all parts, laid end to end along the dimension named above; an argument that names none is the same for every part.
All inputs are finite; a program needn't handle non-finite values.
Results may differ from the reference program's by a relative error of at most 0.0133434.
Values are sent between devices in bfloat16 or wider.
A program may use at most 1 GiB of HBM per device.

```python
import functools
import jax
import jax.numpy as jnp
from jax import lax

N = 512
CZ = 128
CH = 128
LN_EPS = 1e-5


@jax.custom_vjp
def dense_map(x_act, w_mat):
    return jnp.einsum('...k,km->...m', x_act.astype(jnp.float32), w_mat.astype(jnp.float32))


def dense_fwd(x_act, w_mat):
    return dense_map(x_act, w_mat), (x_act, w_mat)


def dense_bwd(saved_res, grad_out):
    x_act, w_mat = saved_res
    grad_b16 = grad_out.astype(jnp.bfloat16).astype(jnp.float32)
    grad_x = jnp.einsum('...m,km->...k', grad_b16, w_mat.astype(jnp.float32)).astype(jnp.bfloat16)
    grad_w = jnp.einsum('...k,...m->km', x_act.astype(jnp.float32), grad_b16).astype(jnp.bfloat16)
    return grad_x, grad_w


dense_map.defvjp(dense_fwd, dense_bwd)


@jax.custom_vjp
def triangle_map(act_a, act_b):
    return jnp.einsum('ikc,jkc->ijc', act_a.astype(jnp.float32), act_b.astype(jnp.float32))


def triangle_fwd(act_a, act_b):
    return triangle_map(act_a, act_b), (act_a, act_b)


def triangle_bwd(saved_res, grad_out):
    act_a, act_b = saved_res
    grad_b16 = grad_out.astype(jnp.bfloat16).astype(jnp.float32)
    grad_a = jnp.einsum('ijc,jkc->ikc', grad_b16, act_b.astype(jnp.float32)).astype(jnp.bfloat16)
    grad_bb = jnp.einsum('ijc,ikc->jkc', grad_b16, act_a.astype(jnp.float32)).astype(jnp.bfloat16)
    return grad_a, grad_bb


triangle_map.defvjp(triangle_fwd, triangle_bwd)


def layer_norm(x_val, ln_scale, ln_offset):
    mean_val = jnp.mean(x_val, axis=-1, keepdims=True)
    centered = x_val - mean_val
    var_val = jnp.mean(centered * centered, axis=-1, keepdims=True)
    return centered * lax.rsqrt(var_val + LN_EPS) * ln_scale.astype(jnp.float32) + ln_offset.astype(jnp.float32)


def outgoing_layer(z_pair, ln_in_scale, ln_in_offset, w_in, b_in, ln_out_scale, ln_out_offset, w_out, b_out, w_gate, b_gate, pair_mask):
    z_f = z_pair.astype(jnp.float32)
    z_norm = layer_norm(z_f, ln_in_scale, ln_in_offset).astype(jnp.bfloat16)
    w_cat = jnp.concatenate([w_in, w_gate], axis=1)
    b_cat = jnp.concatenate([b_in, b_gate]).astype(jnp.float32)
    proj_all = dense_map(z_norm, w_cat) + b_cat
    mask_f = pair_mask.astype(jnp.float32)[..., None]
    proj_a = proj_all[..., :CH]
    proj_b = proj_all[..., CH:2 * CH]
    sig_a = jax.nn.sigmoid(proj_all[..., 2 * CH:3 * CH])
    sig_b = jax.nn.sigmoid(proj_all[..., 3 * CH:4 * CH])
    sig_g = jax.nn.sigmoid(proj_all[..., 4 * CH:])
    act_a = (mask_f * sig_a * proj_a).astype(jnp.bfloat16)
    act_b = (mask_f * sig_b * proj_b).astype(jnp.bfloat16)
    tri_out = triangle_map(act_a, act_b)
    o_norm = layer_norm(tri_out, ln_out_scale, ln_out_offset).astype(jnp.bfloat16)
    update = (dense_map(o_norm, w_out) + b_out.astype(jnp.float32)).astype(jnp.bfloat16)
    return (z_f + sig_g * update.astype(jnp.float32)).astype(jnp.bfloat16)


def setup_inputs(seed: int = 0, part: int = 0) -> dict:
    part_key = jax.random.fold_in(jax.random.key(seed), part)
    k_z, k_dy, k_res, k_pair = jax.random.split(part_key, 4)
    w_keys = jax.random.split(jax.random.key(seed + 1), 12)
    res_keep = (jax.random.randint(k_res, (N,), 0, 8) != 0).astype(jnp.int32)
    pair_keep = (jax.random.randint(k_pair, (N, N), 0, 16) != 0).astype(jnp.int32)
    pair_mask = res_keep[:, None] * res_keep[None, :] * pair_keep
    return {
        'z_pair': jax.random.normal(k_z, (N, N, CZ), jnp.float32).astype(jnp.bfloat16),
        'pair_mask': pair_mask,
        'dz_out': jax.random.normal(k_dy, (N, N, CZ), jnp.float32).astype(jnp.bfloat16),
        'ln_in_scale': (1.0 + 0.3 * jax.random.normal(w_keys[0], (CZ,), jnp.float32)).astype(jnp.bfloat16),
        'ln_in_offset': (0.3 * jax.random.normal(w_keys[1], (CZ,), jnp.float32)).astype(jnp.bfloat16),
        'w_in': (jax.random.normal(w_keys[2], (CZ, 4 * CH), jnp.float32) * CZ ** -0.5).astype(jnp.bfloat16),
        'b_in': (0.5 * jax.random.normal(w_keys[3], (4 * CH,), jnp.float32)).astype(jnp.bfloat16),
        'ln_out_scale': (1.0 + 0.3 * jax.random.normal(w_keys[4], (CH,), jnp.float32)).astype(jnp.bfloat16),
        'ln_out_offset': (0.3 * jax.random.normal(w_keys[5], (CH,), jnp.float32)).astype(jnp.bfloat16),
        'w_out': (jax.random.normal(w_keys[6], (CH, CZ), jnp.float32) * CH ** -0.5).astype(jnp.bfloat16),
        'b_out': (0.5 * jax.random.normal(w_keys[7], (CZ,), jnp.float32)).astype(jnp.bfloat16),
        'w_gate': (jax.random.normal(w_keys[8], (CZ, CZ), jnp.float32) * CZ ** -0.5).astype(jnp.bfloat16),
        'b_gate': (0.5 * jax.random.normal(w_keys[9], (CZ,), jnp.float32)).astype(jnp.bfloat16),
    }


def reference(z_pair, pair_mask, dz_out, ln_in_scale, ln_in_offset, w_in, b_in, ln_out_scale, ln_out_offset, w_out, b_out, w_gate, b_gate):
    layer_fn = functools.partial(outgoing_layer, pair_mask=pair_mask)
    z_next, vjp_fn = jax.vjp(layer_fn, z_pair, ln_in_scale, ln_in_offset, w_in, b_in, ln_out_scale, ln_out_offset, w_out, b_out, w_gate, b_gate)
    d_z, d_in_scale, d_in_offset, d_w_in, d_b_in, d_out_scale, d_out_offset, d_w_out, d_b_out, d_w_gate, d_b_gate = vjp_fn(dz_out)
    return (d_z, d_in_scale, d_in_offset, d_w_in, d_b_in, d_out_scale, d_out_offset, d_w_out, d_b_out, d_w_gate, d_b_gate)
```

```python
import functools
import jax
import jax.numpy as jnp
from jax import lax
from jax.experimental import pallas as pl
from jax.experimental.pallas import tpu as pltpu
from jax.sharding import PartitionSpec as P

LN_EPS = 1e-5
F32 = jnp.float32
BF16 = jnp.bfloat16
LANES = 128
ROWS = 16
CH_STEP = 8
VMEM_LIMIT = 60 * 1024 * 1024


def sigmoid(x_val):
    return 1.0 / (1.0 + jnp.exp(-x_val))


def col_mean(x_val):
    return jnp.sum(x_val, axis=0, keepdims=True) * (1.0 / x_val.shape[0])


def dot_nn(lhs, rhs):
    return jnp.dot(lhs, rhs, preferred_element_type=F32)


def dot_nt(lhs, rhs):
    return lax.dot_general(lhs, rhs, (((1,), (1,)), ((), ())), preferred_element_type=F32)


def dot_tn(lhs, rhs):
    return lax.dot_general(lhs, rhs, (((0,), (0,)), ((), ())), preferred_element_type=F32)


def input_norm(z_rows, scale, offset):
    z_t = jnp.transpose(z_rows.astype(F32))
    centered = z_t - col_mean(z_t)
    inv_std = lax.rsqrt(col_mean(centered * centered) + LN_EPS)
    x_hat = centered * inv_std
    return x_hat, inv_std, (x_hat * scale + offset).astype(BF16)


def project_kernel(keep_norm, z_ref, mask_ref, w_ref, bias_ref, scale_ref, offset_ref, *refs):
    if keep_norm:
        a_ref, b_ref, znt_ref, scr_a, scr_b = refs
    else:
        a_ref, b_ref, scr_a, scr_b = refs
    n_lane = z_ref.shape[1] // LANES
    chans = z_ref.shape[2]
    pitch = ROWS + 1
    plane = chans * pitch

    def row(i, carry):
        for half in range(n_lane // 2):
            cols = slice(half * 256, half * 256 + 256)
            _, _, znt = input_norm(z_ref[i, cols, :], scale_ref[...], offset_ref[...])
            if keep_norm:
                znt_ref[i, :, cols] = znt
            proj = dot_nn(w_ref[...], znt) + bias_ref[...]
            mask_f = jnp.concatenate([mask_ref[i, half * 2 + t] for t in range(2)], axis=1).astype(F32)
            act_a = mask_f * sigmoid(proj[2 * chans:3 * chans]) * proj[:chans]
            act_b = mask_f * sigmoid(proj[3 * chans:]) * proj[chans:2 * chans]
            for t in range(2):
                base = (half * 2 + t) * plane
                part = slice(t * LANES, (t + 1) * LANES)
                scr_a[pl.ds(base + i, chans, stride=pitch), :] = act_a[:, part]
                scr_b[pl.ds(base + i, chans, stride=pitch), :] = act_b[:, part]
        return carry

    lax.fori_loop(0, ROWS, row, 0)

    def pack(c, carry):
        for t in range(n_lane):
            lanes = slice(t * LANES, (t + 1) * LANES)
            at = t * plane + c * pitch
            a_ref[c, :, lanes] = scr_a[pl.ds(at, ROWS), :].astype(BF16)
            b_ref[c, :, lanes] = scr_b[pl.ds(at, ROWS), :].astype(BF16)
        return carry

    lax.fori_loop(0, chans, pack, 0, unroll=4)


def project(z_rows, mask_rows, w_t, bias, scale, offset, keep_norm):
    rows, n_col, chans = z_rows.shape
    full = lambda arr: pl.BlockSpec(arr.shape, lambda s: (0,) * arr.ndim)
    act = jax.ShapeDtypeStruct((chans, rows, n_col), BF16)
    act_spec = pl.BlockSpec((chans, ROWS, n_col), lambda s: (0, s, 0))
    out_shape = [act, act]
    out_specs = [act_spec, act_spec]
    if keep_norm:
        out_shape.append(jax.ShapeDtypeStruct((rows, chans, n_col), BF16))
        out_specs.append(pl.BlockSpec((ROWS, chans, n_col), lambda s: (s, 0, 0)))
    scratch = pltpu.VMEM((n_col // LANES * chans * (ROWS + 1), LANES), F32)
    return pl.pallas_call(
        functools.partial(project_kernel, keep_norm),
        grid=(rows // ROWS,),
        in_specs=[
            pl.BlockSpec((ROWS, n_col, chans), lambda s: (s, 0, 0)),
            pl.BlockSpec((ROWS,) + mask_rows.shape[1:], lambda s: (s, 0, 0, 0)),
            full(w_t), full(bias), full(scale), full(offset)],
        out_specs=out_specs,
        out_shape=out_shape,
        scratch_shapes=[scratch, scratch],
        compiler_params=pltpu.CompilerParams(vmem_limit_bytes=VMEM_LIMIT),
        cost_estimate=pl.CostEstimate(flops=30 * 10 ** 9, bytes_accessed=64 * 2 ** 20, transcendentals=0),
        name='project',
    )(z_rows, mask_rows, w_t, bias, scale, offset)


def middle_kernel(n_mul, n_mid, q_ref, a_ref, b_ref, znt_ref, dy_ref, wg_ref, bg_ref, wo_ref, wot_ref, bo_ref, scale_ref, offset_ref,
                  do_ref, gl_ref, dwo_ref, dwg_ref, vec_ref, scr):
    step = pl.program_id(0)
    tile = LANES
    pitch = tile + 1
    chans = wo_ref.shape[0]

    @pl.when(step == 0)
    def _():
        dwo_ref[...] = jnp.zeros_like(dwo_ref)
        dwg_ref[...] = jnp.zeros_like(dwg_ref)
        vec_ref[...] = jnp.zeros_like(vec_ref)

    @pl.when(step < n_mul)
    def _():
        for j in range(CH_STEP):
            at = (step * CH_STEP + j) * pitch
            scr[pl.ds(at, tile), :] = dot_nt(a_ref[j], b_ref[j])

    @pl.when((step >= n_mul) & (step < n_mul + n_mid))
    def _():
        first = (step - n_mul) * ROWS

        def pair(h, carry):
            r0 = first + 2 * h
            tri = jnp.concatenate([scr[pl.ds(r0 + t, chans, stride=pitch), :] for t in range(2)], axis=1)
            centered = tri - col_mean(tri)
            inv_std = lax.rsqrt(col_mean(centered * centered) + LN_EPS)
            o_hat = centered * inv_std
            o_norm = (o_hat * scale_ref[...] + offset_ref[...]).astype(BF16)
            update = (dot_nn(wot_ref[...], o_norm) + bo_ref[...]).astype(BF16).astype(F32)
            znt = jnp.concatenate([znt_ref[2 * h + t] for t in range(2)], axis=1)
            sig_g = sigmoid(dot_nn(wg_ref[...], znt) + bg_ref[...])
            dy_t = jnp.concatenate([jnp.transpose(dy_ref[2 * h + t].astype(F32)) for t in range(2)], axis=1)
            d_update = (sig_g * dy_t).astype(BF16)
            d_gate = dy_t * update * sig_g * (1.0 - sig_g)
            gate16 = d_gate.astype(BF16)
            d_onorm = dot_nn(wo_ref[...], d_update).astype(BF16).astype(F32)
            grad_hat = d_onorm * scale_ref[...]
            d_tri = inv_std * (grad_hat - col_mean(grad_hat) - o_hat * col_mean(grad_hat * o_hat))
            d_upf = d_update.astype(F32)
            d_sc = d_onorm * o_hat
            for t in range(2):
                part = slice(t * tile, (t + 1) * tile)
                scr[pl.ds(r0 + t, chans, stride=pitch), :] = d_tri[:, part]
                gl_ref[2 * h + t] = gate16[:, part]
            vec_ref[0] += d_sc[:, :tile] + d_sc[:, tile:]
            vec_ref[1] += d_onorm[:, :tile] + d_onorm[:, tile:]
            vec_ref[2] += d_upf[:, :tile] + d_upf[:, tile:]
            vec_ref[3] += d_gate[:, :tile] + d_gate[:, tile:]
            dwo_ref[...] += dot_nt(o_norm, d_update)
            dwg_ref[...] += dot_nt(znt, gate16)
            return carry

        lax.fori_loop(0, ROWS // 2, pair, 0)

    @pl.when(step >= n_mul + n_mid)
    def _():
        for j in range(CH_STEP):
            at = ((step - n_mul - n_mid) * CH_STEP + j) * pitch
            do_ref[j] = scr[pl.ds(at, tile), :].astype(BF16)


def middle(q_idx, act_a, act_b, znt, dy_rows, wg_t, bg, wo, wo_t, bo, scale, offset):
    chans, rows, n_col = act_a.shape
    n_mul = chans // CH_STEP
    n_mid = rows // ROWS
    mul_at = lambda s: jnp.minimum(s, n_mul - 1)
    mid_at = lambda s: jnp.clip(s - n_mul, 0, n_mid - 1)
    out_at = lambda s: jnp.maximum(s - n_mul - n_mid, 0)
    full = lambda shape: pl.BlockSpec(shape, lambda s, q: (0,) * len(shape))
    mats = jax.ShapeDtypeStruct((chans, chans), F32)
    return pl.pallas_call(
        functools.partial(middle_kernel, n_mul, n_mid),
        grid_spec=pltpu.PrefetchScalarGridSpec(
            num_scalar_prefetch=1,
            grid=(2 * n_mul + n_mid,),
            in_specs=[
                pl.BlockSpec((CH_STEP, rows, n_col), lambda s, q: (mul_at(s), 0, 0)),
                pl.BlockSpec((CH_STEP, LANES, n_col), lambda s, q: (mul_at(s), 0, 0)),
                pl.BlockSpec((ROWS, chans, LANES), lambda s, q: (mid_at(s), 0, q[0])),
                pl.BlockSpec((ROWS, LANES, chans), lambda s, q: (mid_at(s), q[0], 0)),
                full(wg_t.shape), full(bg.shape), full(wo.shape), full(wo_t.shape), full(bo.shape), full(scale.shape), full(offset.shape)],
            out_specs=[
                pl.BlockSpec((CH_STEP, rows, LANES), lambda s, q: (out_at(s), 0, 0)),
                pl.BlockSpec((ROWS, chans, LANES), lambda s, q: (mid_at(s), 0, 0)),
                full((chans, chans)), full((chans, chans)), full((4, chans, LANES))],
            scratch_shapes=[pltpu.VMEM((chans * (LANES + 1), LANES), F32)],
        ),
        out_shape=[
            jax.ShapeDtypeStruct((chans, rows, LANES), BF16),
            jax.ShapeDtypeStruct((rows, chans, LANES), BF16),
            mats, mats, jax.ShapeDtypeStruct((4, chans, LANES), F32)],
        compiler_params=pltpu.CompilerParams(vmem_limit_bytes=VMEM_LIMIT),
        cost_estimate=pl.CostEstimate(flops=25 * 10 ** 9, bytes_accessed=48 * 2 ** 20, transcendentals=0),
        name='middle',
    )(q_idx, act_a, act_b, znt, dy_rows, wg_t, bg, wo, wo_t, bo, scale, offset)


def contract_kernel(trans, *refs):
    grads, acts, out_ref = refs[:4], refs[4:8], refs[8]
    for j in range(out_ref.shape[0]):
        rhs = jnp.concatenate([act[j] for act in acts], axis=0)
        if trans:
            lhs = jnp.concatenate([g[j] for g in grads], axis=0)
            out_ref[j] = dot_tn(lhs, rhs).astype(BF16)
        else:
            lhs = jnp.concatenate([g[j] for g in grads], axis=1)
            out_ref[j] = dot_nn(lhs, rhs).astype(BF16)


def contract(grads, acts, trans):
    chans, rows, n_col = acts[0].shape
    step = 4
    return pl.pallas_call(
        functools.partial(contract_kernel, trans),
        grid=(chans // step,),
        in_specs=[pl.BlockSpec((step, rows, LANES), lambda s: (s, 0, 0))] * 4 + [pl.BlockSpec((step, rows, n_col), lambda s: (s, 0, 0))] * 4,
        out_specs=pl.BlockSpec((step, rows, n_col), lambda s: (s, 0, 0)),
        out_shape=jax.ShapeDtypeStruct((chans, rows, n_col), BF16),
        compiler_params=pltpu.CompilerParams(vmem_limit_bytes=VMEM_LIMIT),
        cost_estimate=pl.CostEstimate(flops=15 * 10 ** 9, bytes_accessed=96 * 2 ** 20, transcendentals=0),
        name='contract',
    )(*grads, *acts)


def final_kernel(q_ref, z_ref, mask_ref, dy_ref, da_ref, db_ref, gl0, gl1, gl2, gl3, w_ref, wb_ref, bias_ref, scale_ref, offset_ref,
                 dz_ref, dw_ref, dbin_ref, vec_ref, scr_a, scr_b):
    gls = (gl0, gl1, gl2, gl3)
    chans = z_ref.shape[2]
    n_lane = z_ref.shape[1] // LANES
    pitch = ROWS + 1
    plane = chans * pitch

    @pl.when(pl.program_id(0) == 0)
    def _():
        dw_ref[...] = jnp.zeros_like(dw_ref)
        dbin_ref[...] = jnp.zeros_like(dbin_ref)
        vec_ref[...] = jnp.zeros_like(vec_ref)

    def unpack(c, carry):
        for t in range(n_lane):
            lanes = slice(t * LANES, (t + 1) * LANES)
            at = t * plane + c * pitch
            scr_a[pl.ds(at, ROWS), :] = da_ref[c, :, lanes].astype(F32)
            scr_b[pl.ds(at, ROWS), :] = db_ref[c, :, lanes].astype(F32)
        return carry

    lax.fori_loop(0, chans, unpack, 0, unroll=4)

    def row(i, carry):
        for half in range(n_lane // 2):
            qs = [q_ref[2 * half + t] for t in range(2)]
            offs = [pl.multiple_of(q * LANES, LANES) for q in qs]
            z_rows = jnp.concatenate([z_ref[i, pl.ds(off, LANES), :] for off in offs], axis=0)
            x_hat, inv_std, znt = input_norm(z_rows, scale_ref[...], offset_ref[...])
            proj = dot_nn(w_ref[...], znt) + bias_ref[...]
            mask_f = jnp.concatenate([mask_ref[i, q] for q in qs], axis=1).astype(F32)
            grad_a = jnp.concatenate([scr_a[pl.ds(q * plane + i, chans, stride=pitch), :] for q in qs], axis=1) * mask_f
            grad_b = jnp.concatenate([scr_b[pl.ds(q * plane + i, chans, stride=pitch), :] for q in qs], axis=1) * mask_f
            sig_a = sigmoid(proj[2 * chans:3 * chans])
            sig_b = sigmoid(proj[3 * chans:])
            gs_a = grad_a * sig_a
            gs_b = grad_b * sig_b
            d_proj = jnp.concatenate([gs_a, gs_b, gs_a * proj[:chans] * (1.0 - sig_a), gs_b * proj[chans:2 * chans] * (1.0 - sig_b)], axis=0)
            dbin_ref[...] += d_proj[:, :LANES] + d_proj[:, LANES:]
            gate = jnp.concatenate([gls[2 * half + t][i] for t in range(2)], axis=1)
            grad16 = d_proj.astype(BF16)
            dw_ref[...] += dot_nt(grad16, znt)
            d_znorm = dot_nn(wb_ref[...], jnp.concatenate([grad16, gate], axis=0)).astype(BF16).astype(F32)
            d_sc = d_znorm * x_hat
            vec_ref[0] += d_sc[:, :LANES] + d_sc[:, LANES:]
            vec_ref[1] += d_znorm[:, :LANES] + d_znorm[:, LANES:]
            grad_hat = d_znorm * scale_ref[...]
            d_in = inv_std * (grad_hat - col_mean(grad_hat) - x_hat * col_mean(grad_hat * x_hat))
            d_rows = jnp.transpose(d_in)
            for t in range(2):
                out = d_rows[t * LANES:(t + 1) * LANES] + dy_ref[i, pl.ds(offs[t], LANES), :].astype(F32)
                dz_ref[i, pl.ds(offs[t], LANES), :] = out.astype(BF16)
        return carry

    lax.fori_loop(0, ROWS, row, 0)


def final(q_all, z_rows, mask_rows, dy_rows, d_a, d_b, gates, w_t, w_back, bias, scale, offset):
    rows, n_col, chans = z_rows.shape
    full = lambda shape: pl.BlockSpec(shape, lambda s, q: (0,) * len(shape))
    pair_spec = pl.BlockSpec((ROWS, n_col, chans), lambda s, q: (s, 0, 0))
    act_spec = pl.BlockSpec((chans, ROWS, n_col), lambda s, q: (0, s, 0))
    scratch = pltpu.VMEM((n_col // LANES * chans * (ROWS + 1), LANES), F32)
    return pl.pallas_call(
        final_kernel,
        grid_spec=pltpu.PrefetchScalarGridSpec(
            num_scalar_prefetch=1,
            grid=(rows // ROWS,),
            in_specs=[pair_spec, pl.BlockSpec((ROWS,) + mask_rows.shape[1:], lambda s, q: (s, 0, 0, 0)), pair_spec, act_spec, act_spec]
            + [pl.BlockSpec((ROWS, chans, LANES), lambda s, q: (s, 0, 0))] * 4
            + [full(w_t.shape), full(w_back.shape), full(bias.shape), full(scale.shape), full(offset.shape)],
            out_specs=[pair_spec, full((4 * chans, chans)), full((4 * chans, LANES)), full((2, chans, LANES))],
            scratch_shapes=[scratch, scratch],
        ),
        out_shape=[
            jax.ShapeDtypeStruct(z_rows.shape, BF16),
            jax.ShapeDtypeStruct((4 * chans, chans), F32),
            jax.ShapeDtypeStruct((4 * chans, LANES), F32),
            jax.ShapeDtypeStruct((2, chans, LANES), F32)],
        compiler_params=pltpu.CompilerParams(vmem_limit_bytes=VMEM_LIMIT),
        cost_estimate=pl.CostEstimate(flops=60 * 10 ** 9, bytes_accessed=128 * 2 ** 20, transcendentals=0),
        name='final',
    )(q_all, z_rows, mask_rows, dy_rows, d_a, d_b, *gates, w_t, w_back, bias, scale, offset)


def lane_bcast(vec, width):
    return jnp.broadcast_to(vec.astype(F32)[:, None], (vec.shape[0], width))


def local_grads(z_loc, mask_loc, dy_loc, ln_in_scale, ln_in_offset, w_in, b_in, ln_out_scale, ln_out_offset, w_out, b_out, w_gate, b_gate):
    n_dap = lax.axis_size('dap')
    me = lax.axis_index('dap')
    swap = lambda arr, bit: lax.ppermute(arr, 'dap', [(d, d ^ bit) for d in range(n_dap)])
    w_t = w_in.T
    bias = lane_bcast(b_in, 256)
    in_sc, in_of = lane_bcast(ln_in_scale, 256), lane_bcast(ln_in_offset, 256)
    out_sc, out_of = lane_bcast(ln_out_scale, 256), lane_bcast(ln_out_offset, 256)
    z_far = swap(z_loc, 2)
    mask_loc = mask_loc.reshape(mask_loc.shape[0], -1, 1, LANES)
    mask_far = swap(mask_loc, 2)
    a_0, b_0, znt = project(z_loc, mask_loc, w_t, bias, in_sc, in_of, True)
    a_1, b_1 = swap(a_0, 1), swap(b_0, 1)
    blocks = [me ^ r for r in range(n_dap)]
    mid = lambda r, act_b: middle(blocks[r].astype(jnp.int32)[None], a_0, act_b, znt, dy_loc, w_gate.T, lane_bcast(b_gate, 256),
                                  w_out, w_out.T, lane_bcast(b_out, 256), out_sc, out_of)
    mids = [mid(0, b_0), mid(1, b_1)]
    a_2, b_2 = project(z_far, mask_far, w_t, bias, in_sc, in_of, False)
    b_3, a_3 = swap(b_2, 1), swap(a_2, 1)
    mids += [mid(2, b_2), mid(3, b_3)]
    grads = [m[0] for m in mids]
    d_a = contract(grads, [b_0, b_1, b_2, b_3], False)
    mine = [grads[0]] + [swap(grads[r], r) for r in range(1, n_dap)]
    d_b = contract(mine, [a_0, a_1, a_2, a_3], True)
    w_back = jnp.concatenate([w_in, w_gate], axis=1)
    d_z, dw_t, dbin, vecs = final(jnp.stack(blocks).astype(jnp.int32), z_loc, mask_loc, dy_loc, d_a, d_b, [m[1] for m in mids], w_t, w_back, bias, in_sc, in_of)
    d_wo = sum(m[2] for m in mids)
    d_wg = sum(m[3] for m in mids)
    vec_mid = jnp.sum(sum(m[4] for m in mids), axis=-1)
    vec_in = jnp.sum(vecs, axis=-1)
    summed = lax.psum((vec_in[0], vec_in[1], dw_t, jnp.sum(dbin, axis=-1), vec_mid[0], vec_mid[1], d_wo, vec_mid[2], d_wg, vec_mid[3]), 'dap')
    summed = list(summed)
    summed[2] = summed[2].T
    return (d_z,) + tuple(piece.astype(BF16) for piece in summed)


def solution(mesh):
    pair_spec = P(('batch', 'dap'), None, None)
    mask_spec = P(('batch', 'dap'), None)
    vec_rep = P(None)
    mat_rep = P(None, None)
    vec_part = P('batch')
    mat_part = P('batch', None)
    in_specs = (pair_spec, mask_spec, pair_spec, vec_rep, vec_rep, mat_rep, vec_rep, vec_rep, vec_rep, mat_rep, vec_rep, mat_rep, vec_rep)
    out_specs = (pair_spec, vec_part, vec_part, mat_part, vec_part, vec_part, vec_part, mat_part, vec_part, mat_part, vec_part)
    return jax.shard_map(local_grads, mesh=mesh, in_specs=in_specs, out_specs=out_specs, check_vma=False)
```

```python
import functools
import jax
import jax.numpy as jnp
from jax import lax
from jax.experimental import pallas as pl
from jax.experimental.pallas import tpu as pltpu
from jax.sharding import PartitionSpec as P

LN_EPS = 1e-5
F32 = jnp.float32
BF16 = jnp.bfloat16
LANES = 128
ROWS = 16
CH_STEP = 8
VMEM_LIMIT = 60 * 1024 * 1024


def sigmoid(x_val):
    return 1.0 / (1.0 + jnp.exp(-x_val))


def col_mean(x_val):
    return jnp.sum(x_val, axis=0, keepdims=True) * (1.0 / x_val.shape[0])


def dot_nn(lhs, rhs):
    return jnp.dot(lhs, rhs, preferred_element_type=F32)


def dot_nt(lhs, rhs):
    return lax.dot_general(lhs, rhs, (((1,), (1,)), ((), ())), preferred_element_type=F32)


def dot_tn(lhs, rhs):
    return lax.dot_general(lhs, rhs, (((0,), (0,)), ((), ())), preferred_element_type=F32)


def input_norm(z_rows, scale, offset):
    z_t = jnp.transpose(z_rows.astype(F32))
    centered = z_t - col_mean(z_t)
    inv_std = lax.rsqrt(col_mean(centered * centered) + LN_EPS)
    x_hat = centered * inv_std
    return x_hat, inv_std, (x_hat * scale + offset).astype(BF16)


def project_kernel(keep_norm, z_ref, mask_ref, w_ref, bias_ref, scale_ref, offset_ref, *refs):
    refs = refs[-5:] if keep_norm else refs[-4:]
    a_ref, b_ref = refs[:2]
    scr_a, scr_b = refs[-2:]
    n_lane = z_ref.shape[1] // LANES
    chans = z_ref.shape[2]
    pitch = ROWS + 1
    plane = chans * pitch

    def row(i, carry):
        for half in range(n_lane // 2):
            cols = slice(half * 256, half * 256 + 256)
            _, _, znt = input_norm(z_ref[i, cols, :], scale_ref[...], offset_ref[...])
            if keep_norm:
                refs[2][i, cols, :] = jnp.transpose(znt)
            proj = dot_nn(w_ref[...], znt) + bias_ref[...]
            mask_f = jnp.concatenate([mask_ref[i, half * 2 + t] for t in range(2)], axis=1).astype(F32)
            act_a = mask_f * sigmoid(proj[2 * chans:3 * chans]) * proj[:chans]
            act_b = mask_f * sigmoid(proj[3 * chans:]) * proj[chans:2 * chans]
            for t in range(2):
                base = (half * 2 + t) * plane
                part = slice(t * LANES, (t + 1) * LANES)
                scr_a[pl.ds(base + i, chans, stride=pitch), :] = act_a[:, part]
                scr_b[pl.ds(base + i, chans, stride=pitch), :] = act_b[:, part]
        return carry

    lax.fori_loop(0, ROWS, row, 0)

    def pack(c, carry):
        for t in range(n_lane):
            lanes = slice(t * LANES, (t + 1) * LANES)
            at = t * plane + c * pitch
            a_ref[c, :, lanes] = scr_a[pl.ds(at, ROWS), :].astype(BF16)
            b_ref[c, :, lanes] = scr_b[pl.ds(at, ROWS), :].astype(BF16)
        return carry

    lax.fori_loop(0, chans, pack, 0, unroll=4)


def project(z_rows, mask_rows, first, rows, w_t, bias, scale, offset, keep_norm, after=()):
    _, n_col, chans = z_rows.shape
    z_from, m_from = (0 if z_rows.shape[0] == rows else first // ROWS), first // ROWS
    full = lambda arr: pl.BlockSpec(arr.shape, lambda s: (0,) * arr.ndim)
    act = jax.ShapeDtypeStruct((chans, rows, n_col), BF16)
    act_spec = pl.BlockSpec((chans, ROWS, n_col), lambda s: (0, s, 0))
    out_shape = [act, act]
    out_specs = [act_spec, act_spec]
    pair_spec = pl.BlockSpec((ROWS, n_col, chans), lambda s: (s + z_from, 0, 0))
    if keep_norm:
        out_shape.append(jax.ShapeDtypeStruct((rows, n_col, chans), BF16))
        out_specs.append(pair_spec)
    scratch = pltpu.VMEM((n_col // LANES * chans * (ROWS + 1), LANES), F32)
    return pl.pallas_call(
        functools.partial(project_kernel, keep_norm),
        grid=(rows // ROWS,),
        in_specs=[
            pair_spec,
            pl.BlockSpec((ROWS,) + mask_rows.shape[1:], lambda s: (s + m_from, 0, 0, 0)),
            full(w_t), full(bias), full(scale), full(offset)] + [pl.BlockSpec(memory_space=pl.ANY)] * len(after),
        out_specs=out_specs,
        out_shape=out_shape,
        scratch_shapes=[scratch, scratch],
        compiler_params=pltpu.CompilerParams(vmem_limit_bytes=VMEM_LIMIT),
        cost_estimate=pl.CostEstimate(flops=rows * 2 * 10 ** 8, bytes_accessed=rows * 2 ** 19, transcendentals=0),
        name='project',
    )(z_rows, mask_rows, w_t, bias, scale, offset, *after)


def middle_kernel(n_mul, n_mid, idx_ref, a_ref, b0_ref, b1_ref, zn0_ref, zn1_ref, dy0_ref, dy1_ref, wg_ref, bg_ref, wo_ref, wot_ref, bo_ref, scale_ref, offset_ref, *refs):
    do0_ref, do1_ref, gl_ref, dwo_ref, dwg_ref, vec_ref, scr = refs[-7:]
    step = pl.program_id(0)
    tile = LANES
    half = tile // 2
    pitch = tile + 1
    chans = wo_ref.shape[0]

    @pl.when(step == 0)
    def _():
        dwo_ref[...] = jnp.zeros_like(dwo_ref)
        dwg_ref[...] = jnp.zeros_like(dwg_ref)
        vec_ref[...] = jnp.zeros_like(vec_ref)

    @pl.when(step < n_mul)
    def _():
        for j in range(CH_STEP):
            at = (step * CH_STEP + j) * pitch
            scr[pl.ds(at, tile), :] = dot_nt(a_ref[j], jnp.concatenate([b0_ref[j], b1_ref[j]], axis=0))

    @pl.when((step >= n_mul) & (step < n_mul + n_mid))
    def _():
        first = (step - n_mul) * ROWS

        def pair(h, carry):
            r0 = first + 2 * h
            tri = jnp.concatenate([scr[pl.ds(r0 + t, chans, stride=pitch), :] for t in range(2)], axis=1)
            centered = tri - col_mean(tri)
            inv_std = lax.rsqrt(col_mean(centered * centered) + LN_EPS)
            o_hat = centered * inv_std
            o_norm = (o_hat * scale_ref[...] + offset_ref[...]).astype(BF16)
            update = (dot_nn(wot_ref[...], o_norm) + bo_ref[...]).astype(BF16).astype(F32)
            zn = jnp.concatenate([ref[2 * h + t] for t in range(2) for ref in (zn0_ref, zn1_ref)], axis=0)
            sig_g = sigmoid(dot_nt(wg_ref[...], zn) + bg_ref[...])
            dy_t = jnp.transpose(jnp.concatenate([ref[2 * h + t].astype(F32) for t in range(2) for ref in (dy0_ref, dy1_ref)], axis=0))
            d_update = (sig_g * dy_t).astype(BF16)
            d_gate = dy_t * update * sig_g * (1.0 - sig_g)
            gate16 = d_gate.astype(BF16)
            d_onorm = dot_nn(wo_ref[...], d_update).astype(BF16).astype(F32)
            grad_hat = d_onorm * scale_ref[...]
            d_tri = inv_std * (grad_hat - col_mean(grad_hat) - o_hat * col_mean(grad_hat * o_hat))
            d_upf = d_update.astype(F32)
            d_sc = d_onorm * o_hat
            for t in range(2):
                part = slice(t * tile, (t + 1) * tile)
                scr[pl.ds(r0 + t, chans, stride=pitch), :] = d_tri[:, part]
                gl_ref[2 * h + t] = gate16[:, part]
            vec_ref[0] += d_sc[:, :tile] + d_sc[:, tile:]
            vec_ref[1] += d_onorm[:, :tile] + d_onorm[:, tile:]
            vec_ref[2] += d_upf[:, :tile] + d_upf[:, tile:]
            vec_ref[3] += d_gate[:, :tile] + d_gate[:, tile:]
            dwo_ref[...] += dot_nt(o_norm, d_update)
            dwg_ref[...] += dot_nn(gate16, zn)
            return carry

        lax.fori_loop(0, ROWS // 2, pair, 0)

    @pl.when(step >= n_mul + n_mid)
    def _():
        for j in range(CH_STEP):
            at = ((step - n_mul - n_mid) * CH_STEP + j) * pitch
            do_t = jnp.transpose(scr[pl.ds(at, tile), :]).astype(BF16)
            do0_ref[j] = do_t[:half]
            do1_ref[j] = do_t[half:]


def middle(pieces, act_a, b_parts, zn, dy_rows, wg_t, bg, wo, wo_t, bo, scale, offset, after=()):
    chans, rows, n_col = act_a.shape
    half = LANES // 2
    n_mul = chans // CH_STEP
    n_mid = rows // ROWS
    mul_at = lambda s: jnp.minimum(s, n_mul - 1)
    mid_at = lambda s: jnp.clip(s - n_mul, 0, n_mid - 1)
    out_at = lambda s: jnp.maximum(s - n_mul - n_mid, 0)
    full = lambda shape: pl.BlockSpec(shape, lambda s, q: (0,) * len(shape))
    part_spec = lambda at: pl.BlockSpec((CH_STEP, half, n_col), lambda s, q: (mul_at(s), at, 0))
    piece_spec = lambda n: pl.BlockSpec((ROWS, half, chans), lambda s, q: (mid_at(s), q[n], 0))
    do_spec = pl.BlockSpec((CH_STEP, half, rows), lambda s, q: (out_at(s), 0, 0))
    do_type = jax.ShapeDtypeStruct((chans, half, rows), BF16)
    mats = jax.ShapeDtypeStruct((chans, chans), F32)
    return pl.pallas_call(
        functools.partial(middle_kernel, n_mul, n_mid),
        grid_spec=pltpu.PrefetchScalarGridSpec(
            num_scalar_prefetch=1,
            grid=(2 * n_mul + n_mid,),
            in_specs=[
                pl.BlockSpec((CH_STEP, rows, n_col), lambda s, q: (mul_at(s), 0, 0)),
                part_spec(b_parts[0][1]), part_spec(b_parts[1][1]),
                piece_spec(0), piece_spec(1), piece_spec(0), piece_spec(1),
                full(wg_t.shape), full(bg.shape), full(wo.shape), full(wo_t.shape), full(bo.shape), full(scale.shape), full(offset.shape)]
            + [pl.BlockSpec(memory_space=pl.ANY)] * len(after),
            out_specs=[
                do_spec, do_spec,
                pl.BlockSpec((ROWS, chans, LANES), lambda s, q: (mid_at(s), 0, 0)),
                full((chans, chans)), full((chans, chans)), full((4, chans, LANES))],
            scratch_shapes=[pltpu.VMEM((chans * (LANES + 1), LANES), F32)],
        ),
        out_shape=[
            do_type, do_type,
            jax.ShapeDtypeStruct((rows, chans, LANES), BF16),
            mats, mats, jax.ShapeDtypeStruct((4, chans, LANES), F32)],
        compiler_params=pltpu.CompilerParams(vmem_limit_bytes=VMEM_LIMIT),
        cost_estimate=pl.CostEstimate(flops=25 * 10 ** 9, bytes_accessed=48 * 2 ** 20, transcendentals=0),
        name='middle',
    )(pieces, act_a, b_parts[0][0], b_parts[1][0], zn, zn, dy_rows, dy_rows, wg_t, bg, wo, wo_t, bo, scale, offset, *after)


def grad_a_kernel(n_do, n_act, *refs):
    grads, acts, mask_ref, out_ref = refs[:n_do], refs[n_do:n_do + n_act], refs[n_do + n_act], refs[-1]
    for j in range(out_ref.shape[0]):
        lhs = jnp.concatenate([g[j] for g in grads], axis=0)
        rhs = jnp.concatenate([act[j] for act in acts], axis=0)
        out_ref[j] = (dot_tn(lhs, rhs) * mask_ref[...]).astype(BF16)


def grad_a(grads, acts, mask_f):
    chans, _, rows = grads[0].shape
    n_col = acts[0].shape[2]
    block = lambda arr: pl.BlockSpec((CH_STEP,) + arr.shape[1:], lambda s: (s, 0, 0))
    return pl.pallas_call(
        functools.partial(grad_a_kernel, len(grads), len(acts)),
        grid=(chans // CH_STEP,),
        in_specs=[block(arr) for arr in list(grads) + list(acts)] + [pl.BlockSpec(mask_f.shape, lambda s: (0, 0))],
        out_specs=pl.BlockSpec((CH_STEP, rows, n_col), lambda s: (s, 0, 0)),
        out_shape=jax.ShapeDtypeStruct((chans, rows, n_col), BF16),
        compiler_params=pltpu.CompilerParams(vmem_limit_bytes=VMEM_LIMIT),
        cost_estimate=pl.CostEstimate(flops=15 * 10 ** 9, bytes_accessed=96 * 2 ** 20, transcendentals=0),
        name='grad_a',
    )(*grads, *acts, mask_f)


def grad_b_kernel(n_do, n_act, *refs):
    grads, acts, mask_ref, out_ref = refs[:n_do], refs[n_do:n_do + n_act], refs[n_do + n_act], refs[-1]
    for j in range(out_ref.shape[0]):
        lhs = jnp.concatenate([g[j] for g in grads], axis=1)
        rhs = jnp.concatenate([act[j] for act in acts], axis=0)
        out_ref[j] = (dot_nn(lhs, rhs) * mask_ref[...]).astype(BF16)


def grad_b(grads, acts, mask_f, part, after=()):
    chans, rows, _ = grads[0].shape
    n_col = acts[0].shape[2]
    block = lambda arr: pl.BlockSpec((CH_STEP,) + arr.shape[1:], lambda s: (s, 0, 0))
    return pl.pallas_call(
        functools.partial(grad_b_kernel, len(grads), len(acts)),
        grid=(chans // CH_STEP,),
        in_specs=[block(arr) for arr in list(grads) + list(acts)] + [pl.BlockSpec((rows, n_col), lambda s: (part, 0))]
        + [pl.BlockSpec(memory_space=pl.ANY)] * len(after),
        out_specs=pl.BlockSpec((CH_STEP, rows, n_col), lambda s: (s, 0, 0)),
        out_shape=jax.ShapeDtypeStruct((chans, rows, n_col), BF16),
        compiler_params=pltpu.CompilerParams(vmem_limit_bytes=VMEM_LIMIT),
        cost_estimate=pl.CostEstimate(flops=8 * 10 ** 9, bytes_accessed=76 * 2 ** 20, transcendentals=0),
        name='grad_b',
    )(*grads, *acts, mask_f, *after)


def final_kernel(seeded, q_ref, z_ref, dy_ref, da_ref, db_ref, gl0, gl1, gl2, gl3, w_ref, wb_ref, bias_ref, scale_ref, offset_ref, *refs):
    dz_ref, dw_ref, dbin_ref, vec_ref, scr_a, scr_b = refs[-6:]
    gls = (gl0, gl1, gl2, gl3)
    chans = z_ref.shape[2]
    n_lane = z_ref.shape[1] // LANES
    side = LANES // 2
    pitch = ROWS + 1
    plane = chans * pitch

    @pl.when(pl.program_id(0) == 0)
    def _():
        if seeded:
            for ref, seed in zip((dw_ref, dbin_ref, vec_ref), refs[:3]):
                ref[...] = seed[...]
        else:
            dw_ref[...] = jnp.zeros_like(dw_ref)
            dbin_ref[...] = jnp.zeros_like(dbin_ref)
            vec_ref[...] = jnp.zeros_like(vec_ref)

    def unpack(c, carry):
        for t in range(n_lane):
            lanes = slice(t * LANES, (t + 1) * LANES)
            at = t * plane + c * pitch
            scr_a[pl.ds(at, ROWS), :] = da_ref[c, :, lanes].astype(F32)
            scr_b[pl.ds(at, ROWS), :] = db_ref[c, :, lanes].astype(F32)
        return carry

    lax.fori_loop(0, chans, unpack, 0, unroll=4)

    def row(i, carry):
        for half in range(n_lane // 2):
            qs = [q_ref[2 * half + t] for t in range(2)]
            offs = [pl.multiple_of(q * LANES, LANES) for q in qs]
            z_rows = jnp.concatenate([z_ref[i, pl.ds(off, LANES), :] for off in offs], axis=0)
            x_hat, inv_std, znt = input_norm(z_rows, scale_ref[...], offset_ref[...])
            proj = dot_nn(w_ref[...], znt) + bias_ref[...]
            grad_a = jnp.concatenate([scr_a[pl.ds(q * plane + i, chans, stride=pitch), :] for q in qs], axis=1)
            grad_b = jnp.concatenate([scr_b[pl.ds(q * plane + i, chans, stride=pitch), :] for q in qs], axis=1)
            sig_a = sigmoid(proj[2 * chans:3 * chans])
            sig_b = sigmoid(proj[3 * chans:])
            gs_a = grad_a * sig_a
            gs_b = grad_b * sig_b
            d_proj = jnp.concatenate([gs_a, gs_b, gs_a * proj[:chans] * (1.0 - sig_a), gs_b * proj[chans:2 * chans] * (1.0 - sig_b)], axis=0)
            dbin_ref[...] += d_proj[:, :LANES] + d_proj[:, LANES:]
            gate = [gls[2 * half + t][i] for t in range(2)]
            if half:
                gate = [g[:, part] for part in (slice(0, side), slice(side, LANES)) for g in gate]
            gate = jnp.concatenate(gate, axis=1)
            grad16 = d_proj.astype(BF16)
            dw_ref[...] += dot_nt(grad16, znt)
            d_znorm = dot_nn(wb_ref[...], jnp.concatenate([grad16, gate], axis=0)).astype(BF16).astype(F32)
            d_sc = d_znorm * x_hat
            vec_ref[0] += d_sc[:, :LANES] + d_sc[:, LANES:]
            vec_ref[1] += d_znorm[:, :LANES] + d_znorm[:, LANES:]
            grad_hat = d_znorm * scale_ref[...]
            d_in = inv_std * (grad_hat - col_mean(grad_hat) - x_hat * col_mean(grad_hat * x_hat))
            d_rows = jnp.transpose(d_in)
            for t in range(2):
                out = d_rows[t * LANES:(t + 1) * LANES] + dy_ref[i, pl.ds(offs[t], LANES), :].astype(F32)
                dz_ref[i, pl.ds(offs[t], LANES), :] = out.astype(BF16)
        return carry

    lax.fori_loop(0, ROWS, row, 0)


def final(q_all, z_rows, dy_rows, d_a, d_b, gates, w_t, w_back, bias, scale, offset, first, d_z=None, seeds=()):
    _, n_col, chans = z_rows.shape
    n_step = d_b.shape[1] // ROWS
    at = first // ROWS
    full = lambda shape: pl.BlockSpec(shape, lambda s, q: (0,) * len(shape))
    pair_spec = pl.BlockSpec((ROWS, n_col, chans), lambda s, q: (s + at, 0, 0))
    scratch = pltpu.VMEM((n_col // LANES * chans * (ROWS + 1), LANES), F32)
    sums = [(4 * chans, chans), (4 * chans, LANES), (2, chans, LANES)]
    args = [q_all, z_rows, dy_rows, d_a, d_b, *gates, w_t, w_back, bias, scale, offset, *seeds]
    in_specs = ([pair_spec, pair_spec, pl.BlockSpec((chans, ROWS, n_col), lambda s, q: (0, s + at, 0)),
                 pl.BlockSpec((chans, ROWS, n_col), lambda s, q: (0, s, 0))]
                + [pl.BlockSpec((ROWS, chans, LANES), lambda s, q: (s + at, 0, 0))] * 4
                + [full(w_t.shape), full(w_back.shape), full(bias.shape), full(scale.shape), full(offset.shape)]
                + [full(seed.shape) for seed in seeds])
    alias = {}
    if d_z is not None:
        alias = {len(args): 0}
        args.append(d_z)
        in_specs.append(pl.BlockSpec(memory_space=pl.ANY))
    return pl.pallas_call(
        functools.partial(final_kernel, bool(seeds)),
        grid_spec=pltpu.PrefetchScalarGridSpec(
            num_scalar_prefetch=1,
            grid=(n_step,),
            in_specs=in_specs,
            out_specs=[pair_spec] + [full(shape) for shape in sums],
            scratch_shapes=[scratch, scratch],
        ),
        out_shape=[jax.ShapeDtypeStruct(z_rows.shape, BF16)] + [jax.ShapeDtypeStruct(shape, F32) for shape in sums],
        input_output_aliases=alias,
        compiler_params=pltpu.CompilerParams(vmem_limit_bytes=VMEM_LIMIT),
        cost_estimate=pl.CostEstimate(flops=30 * 10 ** 9, bytes_accessed=64 * 2 ** 20, transcendentals=0),
        name='final',
    )(*args)


def lane_bcast(vec, width):
    return jnp.broadcast_to(vec.astype(F32)[:, None], (vec.shape[0], width))


def local_step(z_loc, mask_loc, dy_loc, ln_in_scale, ln_in_offset, w_in, b_in, ln_out_scale, ln_out_offset, w_out, b_out, w_gate, b_gate):
    n_dap = lax.axis_size('dap')
    me = lax.axis_index('dap')
    swap = lambda arr, bit: lax.ppermute(arr, 'dap', [(d, d ^ bit) for d in range(n_dap)])
    w_t = w_in.T
    bias = lane_bcast(b_in, 256)
    in_sc, in_of = lane_bcast(ln_in_scale, 256), lane_bcast(ln_in_offset, 256)
    out_sc, out_of = lane_bcast(ln_out_scale, 256), lane_bcast(ln_out_offset, 256)
    z_far = swap(z_loc, 2)
    rows = z_loc.shape[0]
    part = rows // 2
    mask_f = mask_loc.astype(F32)
    mask_loc = mask_loc.reshape(rows, -1, 1, LANES)
    mask_far = swap(mask_loc, 2)
    z_far = [swap(z_loc[:part], 2)]
    z_far.append(swap(lax.optimization_barrier(z_loc)[part:], 2))
    weights = (w_t, bias, in_sc, in_of)
    a_0, b_0, zn = project(z_loc, mask_loc, 0, rows, *weights, True)
    b_1 = swap(b_0, 1)
    a_1 = swap(a_0, 1)
    blocks = [me ^ r for r in range(n_dap)]
    tail = (zn, dy_loc, w_gate.T, lane_bcast(b_gate, 256), w_out, w_out.T, lane_bcast(b_out, 256), out_sc, out_of)
    pieces = lambda *vals: jnp.stack(vals).astype(jnp.int32)
    mids = [middle(pieces(2 * blocks[0], 2 * blocks[0] + 1), a_0, [(b_0, 0), (b_0, 1)], *tail)]
    mids.append(middle(pieces(2 * blocks[1], 2 * blocks[1] + 1), a_0, [(b_1, 0), (b_1, 1)], *tail, after=(mids[0][5],)))
    near_out = [swap(mids[1][0], 1), swap(mids[1][1], 1)]
    a_2, b_2, a_3, b_3, far_out = [], [], [], [], []
    for h in range(2):
        a_h, b_h = project(z_far[h], mask_far, h * part, part, *weights, False, after=(mids[-1][5],))
        b_3.append(swap(b_h, 1))
        a_3.append(swap(a_h, 1))
        a_2.append(a_h)
        b_2.append(b_h)
        mids.append(middle(pieces(2 * blocks[2] + h, 2 * blocks[3] + h), a_0, [(b_2[h], 0), (b_3[h], 0)], *tail, after=(a_h,)))
        far_out.append([swap(mids[2 + h][0], 2), swap(mids[2 + h][1], 3)])
    grads = [m[n] for m in mids for n in range(2)]
    d_a = grad_a(grads, [b_0, b_1, b_2[0], b_3[0], b_2[1], b_3[1]], mask_f)
    w_back = jnp.concatenate([w_in, w_gate], axis=1)
    acts = [a_0, a_1, *a_2, *a_3]
    d_z, seeds = None, ()
    for h in range(2):
        d_b = grad_b([mids[0][h], near_out[h], far_out[h][0], far_out[h][1]], acts, mask_f, h, after=(d_a,) if h == 0 else (seeds[2],))
        d_z, *seeds = final(jnp.stack(blocks).astype(jnp.int32), z_loc, dy_loc, d_a, d_b, [m[2] for m in mids], w_t, w_back, bias, in_sc, in_of,
                            h * part, d_z, seeds)
    dw_t, dbin, vecs = seeds
    d_wo = sum(m[3] for m in mids)
    d_wg = sum(m[4] for m in mids).T
    vec_mid = jnp.sum(sum(m[5] for m in mids), axis=-1)
    vec_in = jnp.sum(vecs, axis=-1)
    summed = lax.psum((vec_in[0], vec_in[1], dw_t, jnp.sum(dbin, axis=-1), vec_mid[0], vec_mid[1], d_wo, vec_mid[2], d_wg, vec_mid[3]), 'dap')
    summed = list(summed)
    summed[2] = summed[2].T
    return (d_z,) + tuple(piece.astype(BF16) for piece in summed)


def solution(mesh):
    pair_spec = P(('batch', 'dap'), None, None)
    mask_spec = P(('batch', 'dap'), None)
    vec_rep = P(None)
    mat_rep = P(None, None)
    vec_part = P('batch')
    mat_part = P('batch', None)
    in_specs = (pair_spec, mask_spec, pair_spec, vec_rep, vec_rep, mat_rep, vec_rep, vec_rep, vec_rep, mat_rep, vec_rep, mat_rep, vec_rep)
    out_specs = (pair_spec, vec_part, vec_part, mat_part, vec_part, vec_part, vec_part, mat_part, vec_part, mat_part, vec_part)
    return jax.shard_map(local_step, mesh=mesh, in_specs=in_specs, out_specs=out_specs, check_vma=False)
```

```python
import functools
import jax
import jax.numpy as jnp
from jax import lax
from jax.experimental import pallas as pl
from jax.experimental.pallas import tpu as pltpu
from jax.sharding import PartitionSpec as P

LN_EPS = 1e-5
F32 = jnp.float32
BF16 = jnp.bfloat16
LANES = 128
ROWS = 16
CH_STEP = 8
MID_CH = 16
MID_ROWS = 32
GROUP = 16
VMEM_LIMIT = 60 * 1024 * 1024


def col_mean(x_val):
    return jnp.sum(x_val, axis=0, keepdims=True) * (1.0 / x_val.shape[0])


def dot_nn(lhs, rhs):
    return jnp.dot(lhs, rhs, preferred_element_type=F32)


def dot_nt(lhs, rhs):
    return lax.dot_general(lhs, rhs, (((1,), (1,)), ((), ())), preferred_element_type=F32)


def dot_tn(lhs, rhs):
    return lax.dot_general(lhs, rhs, (((0,), (0,)), ((), ())), preferred_element_type=F32)


def input_norm(z_rows, scale, offset):
    z_t = jnp.transpose(z_rows.astype(F32))
    centered = z_t - col_mean(z_t)
    inv_std = lax.rsqrt(col_mean(centered * centered) + LN_EPS)
    x_hat = centered * inv_std
    return x_hat, inv_std, (x_hat * scale + offset).astype(BF16)


def with_bias(mat, vec):
    pad = jnp.zeros((mat.shape[0], LANES - 1), BF16)
    return jnp.concatenate([mat, vec[:, None], pad], axis=1)


def by_group(arr):
    split = arr.reshape(arr.shape[:-1] + (4, -1, GROUP))
    return jnp.swapaxes(split, -3, -2).reshape(arr.shape)


def from_group(arr):
    split = arr.reshape(arr.shape[:-1] + (-1, 4, GROUP))
    return jnp.swapaxes(split, -3, -2).reshape(arr.shape)


def ones_row(width):
    return (lax.broadcasted_iota(jnp.int32, (LANES, width), 0) == 0).astype(F32).astype(BF16)


def project_kernel(keep_norm, z_ref, mask_ref, w_ref, scale_ref, offset_ref, *refs):
    refs = refs[-5:] if keep_norm else refs[-4:]
    a_ref, b_ref = refs[:2]
    scr_a, scr_b = refs[-2:]
    n_lane = z_ref.shape[1] // LANES
    chans = z_ref.shape[2]
    pitch = ROWS + 1
    plane = chans * pitch
    one16 = ones_row(256)

    def row(i, carry):
        for half in range(n_lane // 2):
            cols = slice(half * 256, half * 256 + 256)
            _, _, znt = input_norm(z_ref[i, cols, :], scale_ref[...], offset_ref[...])
            if keep_norm:
                refs[2][i, cols, :] = jnp.transpose(znt)
            mask16 = jnp.concatenate([mask_ref[i, half * 2 + t] for t in range(2)], axis=1).astype(F32).astype(BF16)
            proj = dot_nn(w_ref[...], jnp.concatenate([znt * mask16, one16 * mask16], axis=0))
            for g in range(chans // GROUP):
                pa, pb, la, lb = [proj[(4 * g + n) * GROUP:(4 * g + n + 1) * GROUP] for n in range(4)]
                for scr, val in ((scr_a, jax.nn.sigmoid(la) * pa), (scr_b, jax.nn.sigmoid(lb) * pb)):
                    for t in range(2):
                        at = (half * 2 + t) * plane + g * GROUP * pitch + i
                        scr[pl.ds(at, GROUP, stride=pitch), :] = val[:, t * LANES:(t + 1) * LANES]
        return carry

    lax.fori_loop(0, ROWS, row, 0)

    def pack(c, carry):
        for t in range(n_lane):
            lanes = slice(t * LANES, (t + 1) * LANES)
            at = t * plane + c * pitch
            a_ref[c, :, lanes] = scr_a[pl.ds(at, ROWS), :].astype(BF16)
            b_ref[c, :, lanes] = scr_b[pl.ds(at, ROWS), :].astype(BF16)
        return carry

    lax.fori_loop(0, chans, pack, 0, unroll=4)


def project(z_rows, mask_rows, first, rows, w_t, scale, offset, keep_norm, after=()):
    _, n_col, chans = z_rows.shape
    z_from, m_from = (0 if z_rows.shape[0] == rows else first // ROWS), first // ROWS
    full = lambda arr: pl.BlockSpec(arr.shape, lambda s: (0,) * arr.ndim)
    act = jax.ShapeDtypeStruct((chans, rows, n_col), BF16)
    act_spec = pl.BlockSpec((chans, ROWS, n_col), lambda s: (0, s, 0))
    out_shape = [act, act]
    out_specs = [act_spec, act_spec]
    pair_spec = pl.BlockSpec((ROWS, n_col, chans), lambda s: (s + z_from, 0, 0))
    if keep_norm:
        out_shape.append(jax.ShapeDtypeStruct((rows, n_col, chans), BF16))
        out_specs.append(pair_spec)
    scratch = pltpu.VMEM((n_col // LANES * chans * (ROWS + 1), LANES), F32)
    return pl.pallas_call(
        functools.partial(project_kernel, keep_norm),
        grid=(rows // ROWS,),
        in_specs=[
            pair_spec,
            pl.BlockSpec((ROWS,) + mask_rows.shape[1:], lambda s: (s + m_from, 0, 0, 0)),
            full(w_t), full(scale), full(offset)] + [pl.BlockSpec(memory_space=pl.ANY)] * len(after),
        out_specs=out_specs,
        out_shape=out_shape,
        scratch_shapes=[scratch, scratch],
        compiler_params=pltpu.CompilerParams(vmem_limit_bytes=VMEM_LIMIT),
        cost_estimate=pl.CostEstimate(flops=rows * 2 * 10 ** 8, bytes_accessed=rows * 2 ** 19, transcendentals=0),
        name='project',
    )(z_rows, mask_rows, w_t, scale, offset, *after)


def middle_kernel(n_mul, n_mid, idx_ref, a_ref, b0_ref, b1_ref, zn0_ref, zn1_ref, dy0_ref, dy1_ref, wg_ref, wo_ref, wot_ref, scale_ref, offset_ref, *refs):
    do0_ref, do1_ref, gl_ref, dwo_ref, dwg_ref, vec_ref, scr = refs[-7:]
    step = pl.program_id(0)
    tile = LANES
    half = tile // 2
    pitch = tile + 1
    chans = wo_ref.shape[0]

    one16 = ones_row(2 * tile)
    one_col = (lax.broadcasted_iota(jnp.int32, (2 * tile, LANES), 1) == 0).astype(F32).astype(BF16)

    @pl.when(step == 0)
    def _():
        dwo_ref[...] = jnp.zeros_like(dwo_ref)
        dwg_ref[...] = jnp.zeros_like(dwg_ref)
        vec_ref[...] = jnp.zeros_like(vec_ref)

    @pl.when(step < n_mul)
    def _():
        for j in range(MID_CH):
            at = (step * MID_CH + j) * pitch
            scr[pl.ds(at, tile), :] = dot_nt(a_ref[j], jnp.concatenate([b0_ref[j], b1_ref[j]], axis=0))

    @pl.when((step >= n_mul) & (step < n_mul + n_mid))
    def _():
        first = (step - n_mul) * MID_ROWS

        def pair(h, carry):
            r0 = first + 2 * h
            tri = jnp.concatenate([scr[pl.ds(r0 + t, chans, stride=pitch), :] for t in range(2)], axis=1)
            centered = tri - col_mean(tri)
            inv_std = lax.rsqrt(col_mean(centered * centered) + LN_EPS)
            o_hat = centered * inv_std
            o_norm = (o_hat * scale_ref[...] + offset_ref[...]).astype(BF16)
            update = dot_nn(wot_ref[...], jnp.concatenate([o_norm, one16], axis=0)).astype(BF16).astype(F32)
            zn = jnp.concatenate([ref[2 * h + t] for t in range(2) for ref in (zn0_ref, zn1_ref)], axis=0)
            sig_g = jax.nn.sigmoid(dot_nt(wg_ref[...], jnp.concatenate([zn, one_col], axis=1)))
            dy_t = jnp.transpose(jnp.concatenate([ref[2 * h + t].astype(F32) for t in range(2) for ref in (dy0_ref, dy1_ref)], axis=0))
            d_update = (sig_g * dy_t).astype(BF16)
            d_gate = dy_t * update * sig_g * (1.0 - sig_g)
            gate16 = d_gate.astype(BF16)
            d_onorm = dot_nn(wo_ref[...], d_update).astype(BF16).astype(F32)
            grad_hat = d_onorm * scale_ref[...]
            d_tri = inv_std * (grad_hat - col_mean(grad_hat) - o_hat * col_mean(grad_hat * o_hat))
            d_upf = d_update.astype(F32)
            d_sc = d_onorm * o_hat
            for t in range(2):
                part = slice(t * tile, (t + 1) * tile)
                scr[pl.ds(r0 + t, chans, stride=pitch), :] = d_tri[:, part]
                gl_ref[2 * h + t] = gate16[:, part]
            vec_ref[0] += d_sc[:, :tile] + d_sc[:, tile:]
            vec_ref[1] += d_onorm[:, :tile] + d_onorm[:, tile:]
            vec_ref[2] += d_upf[:, :tile] + d_upf[:, tile:]
            vec_ref[3] += d_gate[:, :tile] + d_gate[:, tile:]
            dwo_ref[...] += dot_nt(o_norm, d_update)
            dwg_ref[...] += dot_nn(gate16, zn)
            return carry

        lax.fori_loop(0, MID_ROWS // 2, pair, 0)

    @pl.when(step >= n_mul + n_mid)
    def _():
        for j in range(MID_CH):
            at = ((step - n_mul - n_mid) * MID_CH + j) * pitch
            do_t = jnp.transpose(scr[pl.ds(at, tile), :]).astype(BF16)
            do0_ref[j] = do_t[:half]
            do1_ref[j] = do_t[half:]


def middle(pieces, act_a, b_parts, zn, dy_rows, wg_t, wo, wo_t, scale, offset, after=()):
    chans, rows, n_col = act_a.shape
    half = LANES // 2
    n_mul = chans // MID_CH
    n_mid = rows // MID_ROWS
    mul_at = lambda s: jnp.minimum(s, n_mul - 1)
    mid_at = lambda s: jnp.clip(s - n_mul, 0, n_mid - 1)
    out_at = lambda s: jnp.maximum(s - n_mul - n_mid, 0)
    full = lambda shape: pl.BlockSpec(shape, lambda s, q: (0,) * len(shape))
    part_spec = lambda at: pl.BlockSpec((MID_CH, half, n_col), lambda s, q: (mul_at(s), at, 0))
    piece_spec = lambda n: pl.BlockSpec((MID_ROWS, half, chans), lambda s, q: (mid_at(s), q[n], 0))
    do_spec = pl.BlockSpec((MID_CH, half, rows), lambda s, q: (out_at(s), 0, 0))
    do_type = jax.ShapeDtypeStruct((chans, half, rows), BF16)
    mats = jax.ShapeDtypeStruct((chans, chans), F32)
    return pl.pallas_call(
        functools.partial(middle_kernel, n_mul, n_mid),
        grid_spec=pltpu.PrefetchScalarGridSpec(
            num_scalar_prefetch=1,
            grid=(2 * n_mul + n_mid,),
            in_specs=[
                pl.BlockSpec((MID_CH, rows, n_col), lambda s, q: (mul_at(s), 0, 0)),
                part_spec(b_parts[0][1]), part_spec(b_parts[1][1]),
                piece_spec(0), piece_spec(1), piece_spec(0), piece_spec(1),
                full(wg_t.shape), full(wo.shape), full(wo_t.shape), full(scale.shape), full(offset.shape)]
            + [pl.BlockSpec(memory_space=pl.ANY)] * len(after),
            out_specs=[
                do_spec, do_spec,
                pl.BlockSpec((MID_ROWS, chans, LANES), lambda s, q: (mid_at(s), 0, 0)),
                full((chans, chans)), full((chans, chans)), full((4, chans, LANES))],
            scratch_shapes=[pltpu.VMEM((chans * (LANES + 1), LANES), F32)],
        ),
        out_shape=[
            do_type, do_type,
            jax.ShapeDtypeStruct((rows, chans, LANES), BF16),
            mats, mats, jax.ShapeDtypeStruct((4, chans, LANES), F32)],
        compiler_params=pltpu.CompilerParams(vmem_limit_bytes=VMEM_LIMIT),
        cost_estimate=pl.CostEstimate(flops=25 * 10 ** 9, bytes_accessed=48 * 2 ** 20, transcendentals=0),
        name='middle',
    )(pieces, act_a, b_parts[0][0], b_parts[1][0], zn, zn, dy_rows, dy_rows, wg_t, wo, wo_t, scale, offset, *after)


def grad_a_kernel(n_do, n_act, *refs):
    grads, acts, mask_ref, out_ref = refs[:n_do], refs[n_do:n_do + n_act], refs[n_do + n_act], refs[-1]
    for j in range(out_ref.shape[0]):
        lhs = jnp.concatenate([g[j] for g in grads], axis=0)
        rhs = jnp.concatenate([act[j] for act in acts], axis=0)
        out_ref[j] = (dot_tn(lhs, rhs) * mask_ref[...]).astype(BF16)


def grad_a(grads, acts, mask_f):
    chans, _, rows = grads[0].shape
    n_col = acts[0].shape[2]
    block = lambda arr: pl.BlockSpec((CH_STEP,) + arr.shape[1:], lambda s: (s, 0, 0))
    return pl.pallas_call(
        functools.partial(grad_a_kernel, len(grads), len(acts)),
        grid=(chans // CH_STEP,),
        in_specs=[block(arr) for arr in list(grads) + list(acts)] + [pl.BlockSpec(mask_f.shape, lambda s: (0, 0))],
        out_specs=pl.BlockSpec((CH_STEP, rows, n_col), lambda s: (s, 0, 0)),
        out_shape=jax.ShapeDtypeStruct((chans, rows, n_col), BF16),
        compiler_params=pltpu.CompilerParams(vmem_limit_bytes=VMEM_LIMIT),
        cost_estimate=pl.CostEstimate(flops=15 * 10 ** 9, bytes_accessed=96 * 2 ** 20, transcendentals=0),
        name='grad_a',
    )(*grads, *acts, mask_f)


def grad_b_kernel(n_do, n_act, *refs):
    grads, acts, mask_ref, out_ref = refs[:n_do], refs[n_do:n_do + n_act], refs[n_do + n_act], refs[-1]
    for j in range(out_ref.shape[0]):
        lhs = jnp.concatenate([g[j] for g in grads], axis=1)
        rhs = jnp.concatenate([act[j] for act in acts], axis=0)
        out_ref[j] = (dot_nn(lhs, rhs) * mask_ref[...]).astype(BF16)


def grad_b(grads, acts, mask_f, part, after=()):
    chans, rows, _ = grads[0].shape
    n_col = acts[0].shape[2]
    block = lambda arr: pl.BlockSpec((CH_STEP,) + arr.shape[1:], lambda s: (s, 0, 0))
    return pl.pallas_call(
        functools.partial(grad_b_kernel, len(grads), len(acts)),
        grid=(chans // CH_STEP,),
        in_specs=[block(arr) for arr in list(grads) + list(acts)] + [pl.BlockSpec((rows, n_col), lambda s: (part, 0))]
        + [pl.BlockSpec(memory_space=pl.ANY)] * len(after),
        out_specs=pl.BlockSpec((CH_STEP, rows, n_col), lambda s: (s, 0, 0)),
        out_shape=jax.ShapeDtypeStruct((chans, rows, n_col), BF16),
        compiler_params=pltpu.CompilerParams(vmem_limit_bytes=VMEM_LIMIT),
        cost_estimate=pl.CostEstimate(flops=8 * 10 ** 9, bytes_accessed=76 * 2 ** 20, transcendentals=0),
        name='grad_b',
    )(*grads, *acts, mask_f, *after)


def final_kernel(seeded, q_ref, z_ref, dy_ref, da_ref, db_ref, gl0, gl1, gl2, gl3, w_ref, wb_ref, scale_ref, offset_ref, *refs):
    dz_ref, dw_ref, dbin_ref, vec_ref, scr_a, scr_b = refs[-6:]
    gls = (gl0, gl1, gl2, gl3)
    chans = z_ref.shape[2]
    n_lane = z_ref.shape[1] // LANES
    side = LANES // 2
    pitch = ROWS + 1
    plane = chans * pitch

    @pl.when(pl.program_id(0) == 0)
    def _():
        if seeded:
            for ref, seed in zip((dw_ref, dbin_ref, vec_ref), refs[:3]):
                ref[...] = seed[...]
        else:
            dw_ref[...] = jnp.zeros_like(dw_ref)
            dbin_ref[...] = jnp.zeros_like(dbin_ref)
            vec_ref[...] = jnp.zeros_like(vec_ref)

    one16 = ones_row(n_lane * LANES)

    def unpack(c, carry):
        for t in range(n_lane):
            lanes = slice(t * LANES, (t + 1) * LANES)
            at = t * plane + c * pitch
            scr_a[pl.ds(at, ROWS), :] = da_ref[c, :, lanes].astype(F32)
            scr_b[pl.ds(at, ROWS), :] = db_ref[c, :, lanes].astype(F32)
        return carry

    lax.fori_loop(0, chans, unpack, 0, unroll=4)

    def row(i, carry):
        qs = [q_ref[t] for t in range(n_lane)]
        offs = [pl.multiple_of(q * LANES, LANES) for q in qs]
        fold = lambda val: sum(val[:, t * LANES:(t + 1) * LANES] for t in range(n_lane))
        z_rows = jnp.concatenate([z_ref[i, pl.ds(off, LANES), :] for off in offs], axis=0)
        x_hat, inv_std, znt = input_norm(z_rows, scale_ref[...], offset_ref[...])
        proj = dot_nn(w_ref[...], jnp.concatenate([znt, one16], axis=0))
        grad16 = []
        for g in range(chans // GROUP):
            parts = [proj[(4 * g + n) * GROUP:(4 * g + n + 1) * GROUP] for n in range(4)]
            vals = [None] * 4
            for n, scr in enumerate((scr_a, scr_b)):
                grad = jnp.concatenate([scr[pl.ds(q * plane + g * GROUP * pitch + i, GROUP, stride=pitch), :] for q in qs], axis=1)
                sig = jax.nn.sigmoid(parts[2 + n])
                vals[n] = grad * sig
                vals[2 + n] = vals[n] * parts[n] * (1.0 - sig)
            for n in range(4):
                dbin_ref[(4 * g + n) * GROUP:(4 * g + n + 1) * GROUP] += fold(vals[n])
                grad16.append(vals[n].astype(BF16))
        grad16 = jnp.concatenate(grad16, axis=0)
        gate = [g[i] for g in gls[:2]] + [g[i][:, part] for part in (slice(0, side), slice(side, LANES)) for g in gls[2:]]
        gate = jnp.concatenate(gate, axis=1)
        dw_ref[...] += dot_nt(znt, grad16)
        d_znorm = dot_nn(wb_ref[...], jnp.concatenate([grad16, gate], axis=0)).astype(BF16).astype(F32)
        vec_ref[0] += fold(d_znorm * x_hat)
        vec_ref[1] += fold(d_znorm)
        grad_hat = d_znorm * scale_ref[...]
        d_in = inv_std * (grad_hat - col_mean(grad_hat) - x_hat * col_mean(grad_hat * x_hat))
        d_rows = jnp.transpose(d_in)
        for t in range(n_lane):
            out = d_rows[t * LANES:(t + 1) * LANES] + dy_ref[i, pl.ds(offs[t], LANES), :].astype(F32)
            dz_ref[i, pl.ds(offs[t], LANES), :] = out.astype(BF16)
        return carry

    lax.fori_loop(0, ROWS, row, 0)


def final(q_all, z_rows, dy_rows, d_a, d_b, gates, w_t, w_back, scale, offset, first, d_z=None, seeds=()):
    _, n_col, chans = z_rows.shape
    n_step = d_b.shape[1] // ROWS
    at = first // ROWS
    full = lambda shape: pl.BlockSpec(shape, lambda s, q: (0,) * len(shape))
    pair_spec = pl.BlockSpec((ROWS, n_col, chans), lambda s, q: (s + at, 0, 0))
    scratch = pltpu.VMEM((n_col // LANES * chans * (ROWS + 1), LANES), F32)
    sums = [(chans, 4 * chans), (4 * chans, LANES), (2, chans, LANES)]
    args = [q_all, z_rows, dy_rows, d_a, d_b, *gates, w_t, w_back, scale, offset, *seeds]
    in_specs = ([pair_spec, pair_spec, pl.BlockSpec((chans, ROWS, n_col), lambda s, q: (0, s + at, 0)),
                 pl.BlockSpec((chans, ROWS, n_col), lambda s, q: (0, s, 0))]
                + [pl.BlockSpec((ROWS, chans, LANES), lambda s, q: (s + at, 0, 0))] * 4
                + [full(w_t.shape), full(w_back.shape), full(scale.shape), full(offset.shape)]
                + [full(seed.shape) for seed in seeds])
    alias = {}
    if d_z is not None:
        alias = {len(args): 0}
        args.append(d_z)
        in_specs.append(pl.BlockSpec(memory_space=pl.ANY))
    return pl.pallas_call(
        functools.partial(final_kernel, bool(seeds)),
        grid_spec=pltpu.PrefetchScalarGridSpec(
            num_scalar_prefetch=1,
            grid=(n_step,),
            in_specs=in_specs,
            out_specs=[pair_spec] + [full(shape) for shape in sums],
            scratch_shapes=[scratch, scratch],
        ),
        out_shape=[jax.ShapeDtypeStruct(z_rows.shape, BF16)] + [jax.ShapeDtypeStruct(shape, F32) for shape in sums],
        input_output_aliases=alias,
        compiler_params=pltpu.CompilerParams(vmem_limit_bytes=VMEM_LIMIT),
        cost_estimate=pl.CostEstimate(flops=30 * 10 ** 9, bytes_accessed=64 * 2 ** 20, transcendentals=0),
        name='final',
    )(*args)


def lane_bcast(vec, width):
    return jnp.broadcast_to(vec.astype(F32)[:, None], (vec.shape[0], width))


def local_step(z_loc, mask_loc, dy_loc, ln_in_scale, ln_in_offset, w_in, b_in, ln_out_scale, ln_out_offset, w_out, b_out, w_gate, b_gate):
    n_dap = lax.axis_size('dap')
    me = lax.axis_index('dap')
    swap = lambda arr, bit: lax.ppermute(arr, 'dap', [(d, d ^ bit) for d in range(n_dap)])
    w_t = with_bias(by_group(w_in).T, by_group(b_in))
    row_sc, row_of = (lane_bcast(v, z_loc.shape[1]) for v in (ln_in_scale, ln_in_offset))
    in_sc, in_of = lane_bcast(ln_in_scale, 256), lane_bcast(ln_in_offset, 256)
    out_sc, out_of = lane_bcast(ln_out_scale, 256), lane_bcast(ln_out_offset, 256)
    z_far = swap(z_loc, 2)
    rows = z_loc.shape[0]
    part = rows // 2
    mask_f = mask_loc.astype(F32)
    mask_loc = mask_loc.reshape(rows, -1, 1, LANES)
    mask_far = swap(mask_loc, 2)
    z_far = [swap(z_loc[:part], 2)]
    z_far.append(swap(lax.optimization_barrier(z_loc)[part:], 2))
    weights = (w_t, in_sc, in_of)
    a_0, b_0, zn = project(z_loc, mask_loc, 0, rows, *weights, True)
    b_1 = swap(b_0, 1)
    a_1 = swap(a_0, 1)
    blocks = [me ^ r for r in range(n_dap)]
    tail = (zn, dy_loc, with_bias(w_gate.T, b_gate), w_out, with_bias(w_out.T, b_out), out_sc, out_of)
    pieces = lambda *vals: jnp.stack(vals).astype(jnp.int32)
    mids = [middle(pieces(2 * blocks[0], 2 * blocks[0] + 1), a_0, [(b_0, 0), (b_0, 1)], *tail)]
    mids.append(middle(pieces(2 * blocks[1], 2 * blocks[1] + 1), a_0, [(b_1, 0), (b_1, 1)], *tail, after=(mids[0][5],)))
    near_out = [swap(mids[1][0], 1), swap(mids[1][1], 1)]
    a_2, b_2, a_3, b_3, far_out = [], [], [], [], []
    for h in range(2):
        a_h, b_h = project(z_far[h], mask_far, h * part, part, *weights, False, after=(mids[-1][5],))
        b_3.append(swap(b_h, 1))
        a_3.append(swap(a_h, 1))
        a_2.append(a_h)
        b_2.append(b_h)
        mids.append(middle(pieces(2 * blocks[2] + h, 2 * blocks[3] + h), a_0, [(b_2[h], 0), (b_3[h], 0)], *tail, after=(a_h,)))
        far_out.append([swap(mids[2 + h][0], 2), swap(mids[2 + h][1], 3)])
    grads = [m[n] for m in mids for n in range(2)]
    d_a = grad_a(grads, [b_0, b_1, b_2[0], b_3[0], b_2[1], b_3[1]], mask_f)
    w_back = jnp.concatenate([by_group(w_in), w_gate], axis=1)
    acts = [a_0, a_1, *a_2, *a_3]
    d_z, seeds = None, ()
    for h in range(2):
        d_b = grad_b([mids[0][h], near_out[h], far_out[h][0], far_out[h][1]], acts, mask_f, h, after=(d_a,) if h == 0 else (seeds[2],))
        d_z, *seeds = final(jnp.stack(blocks).astype(jnp.int32), z_loc, dy_loc, d_a, d_b, [m[2] for m in mids], w_t, w_back, row_sc, row_of,
                            h * part, d_z, seeds)
    dw_t, dbin, vecs = seeds
    d_wo = sum(m[3] for m in mids)
    d_wg = sum(m[4] for m in mids).T
    vec_mid = jnp.sum(sum(m[5] for m in mids), axis=-1)
    vec_in = jnp.sum(vecs, axis=-1)
    summed = lax.psum((vec_in[0], vec_in[1], dw_t, jnp.sum(dbin, axis=-1), vec_mid[0], vec_mid[1], d_wo, vec_mid[2], d_wg, vec_mid[3]), 'dap')
    summed = list(summed)
    summed[2] = from_group(summed[2])
    summed[3] = from_group(summed[3])
    return (d_z,) + tuple(piece.astype(BF16) for piece in summed)


def solution(mesh):
    pair_spec = P(('batch', 'dap'), None, None)
    mask_spec = P(('batch', 'dap'), None)
    vec_rep = P(None)
    mat_rep = P(None, None)
    vec_part = P('batch')
    mat_part = P('batch', None)
    in_specs = (pair_spec, mask_spec, pair_spec, vec_rep, vec_rep, mat_rep, vec_rep, vec_rep, vec_rep, mat_rep, vec_rep, mat_rep, vec_rep)
    out_specs = (pair_spec, vec_part, vec_part, mat_part, vec_part, vec_part, vec_part, mat_part, vec_part, mat_part, vec_part)
    return jax.shard_map(local_step, mesh=mesh, in_specs=in_specs, out_specs=out_specs, check_vma=False)
```

```python
import functools
import jax
import jax.numpy as jnp
from jax import lax
from jax.experimental import pallas as pl
from jax.experimental.pallas import tpu as pltpu
from jax.sharding import PartitionSpec as P

LN_EPS = 1e-5
F32 = jnp.float32
BF16 = jnp.bfloat16
LANES = 128
ROWS = 16
MID_CH = 16
MID_ROWS = 32
GROUP = 16
VMEM_LIMIT = 60 * 1024 * 1024


def col_mean(x_val):
    return jnp.sum(x_val, axis=0, keepdims=True) * (1.0 / x_val.shape[0])


def dot_nn(lhs, rhs):
    return jnp.dot(lhs, rhs, preferred_element_type=F32)


def dot_nt(lhs, rhs):
    return lax.dot_general(lhs, rhs, (((1,), (1,)), ((), ())), preferred_element_type=F32)


def dot_tn(lhs, rhs):
    return lax.dot_general(lhs, rhs, (((0,), (0,)), ((), ())), preferred_element_type=F32)


def input_norm(z_rows, scale, offset):
    z_t = jnp.transpose(z_rows.astype(F32))
    centered = z_t - col_mean(z_t)
    inv_std = lax.rsqrt(col_mean(centered * centered) + LN_EPS)
    x_hat = centered * inv_std
    return x_hat, inv_std, (x_hat * scale + offset).astype(BF16)


def with_bias(mat, vec):
    pad = jnp.zeros((mat.shape[0], LANES - 1), BF16)
    return jnp.concatenate([mat, vec[:, None], pad], axis=1)


def by_group(arr):
    split = arr.reshape(arr.shape[:-1] + (4, -1, GROUP))
    return jnp.swapaxes(split, -3, -2).reshape(arr.shape)


def from_group(arr):
    split = arr.reshape(arr.shape[:-1] + (-1, 4, GROUP))
    return jnp.swapaxes(split, -3, -2).reshape(arr.shape)


def ones_row(width):
    return (lax.broadcasted_iota(jnp.int32, (LANES, width), 0) == 0).astype(F32).astype(BF16)


def project_kernel(keep_norm, z_ref, mask_ref, w_ref, scale_ref, offset_ref, *refs):
    refs = refs[-5:] if keep_norm else refs[-4:]
    a_ref, b_ref = refs[:2]
    scr_a, scr_b = refs[-2:]
    n_lane = z_ref.shape[1] // LANES
    chans = z_ref.shape[2]
    pitch = ROWS + 1
    plane = chans * pitch
    one16 = ones_row(256)

    def row(i, carry):
        for half in range(n_lane // 2):
            cols = slice(half * 256, half * 256 + 256)
            _, _, znt = input_norm(z_ref[i, cols, :], scale_ref[...], offset_ref[...])
            if keep_norm:
                refs[2][i, cols, :] = jnp.transpose(znt)
            mask16 = jnp.concatenate([mask_ref[i, half * 2 + t] for t in range(2)], axis=1).astype(F32).astype(BF16)
            proj = dot_nn(w_ref[...], jnp.concatenate([znt * mask16, one16 * mask16], axis=0))
            for g in range(chans // GROUP):
                pa, pb, la, lb = [proj[(4 * g + n) * GROUP:(4 * g + n + 1) * GROUP] for n in range(4)]
                for scr, val in ((scr_a, jax.nn.sigmoid(la) * pa), (scr_b, jax.nn.sigmoid(lb) * pb)):
                    for t in range(2):
                        at = (half * 2 + t) * plane + g * GROUP * pitch + i
                        scr[pl.ds(at, GROUP, stride=pitch), :] = val[:, t * LANES:(t + 1) * LANES]
        return carry

    lax.fori_loop(0, ROWS, row, 0)

    def pack(c, carry):
        for t in range(n_lane):
            lanes = slice(t * LANES, (t + 1) * LANES)
            at = t * plane + c * pitch
            a_ref[c, :, lanes] = scr_a[pl.ds(at, ROWS), :].astype(BF16)
            b_ref[c, :, lanes] = scr_b[pl.ds(at, ROWS), :].astype(BF16)
        return carry

    lax.fori_loop(0, chans, pack, 0, unroll=4)


def project(z_rows, mask_rows, first, rows, w_t, scale, offset, keep_norm, after=()):
    _, n_col, chans = z_rows.shape
    z_from, m_from = (0 if z_rows.shape[0] == rows else first // ROWS), first // ROWS
    full = lambda arr: pl.BlockSpec(arr.shape, lambda s: (0,) * arr.ndim)
    act = jax.ShapeDtypeStruct((chans, rows, n_col), BF16)
    act_spec = pl.BlockSpec((chans, ROWS, n_col), lambda s: (0, s, 0))
    out_shape = [act, act]
    out_specs = [act_spec, act_spec]
    pair_spec = pl.BlockSpec((ROWS, n_col, chans), lambda s: (s + z_from, 0, 0))
    if keep_norm:
        out_shape.append(jax.ShapeDtypeStruct((rows, n_col, chans), BF16))
        out_specs.append(pair_spec)
    scratch = pltpu.VMEM((n_col // LANES * chans * (ROWS + 1), LANES), F32)
    return pl.pallas_call(
        functools.partial(project_kernel, keep_norm),
        grid=(rows // ROWS,),
        in_specs=[
            pair_spec,
            pl.BlockSpec((ROWS,) + mask_rows.shape[1:], lambda s: (s + m_from, 0, 0, 0)),
            full(w_t), full(scale), full(offset)] + [pl.BlockSpec(memory_space=pl.ANY)] * len(after),
        out_specs=out_specs,
        out_shape=out_shape,
        scratch_shapes=[scratch, scratch],
        compiler_params=pltpu.CompilerParams(vmem_limit_bytes=VMEM_LIMIT),
        cost_estimate=pl.CostEstimate(flops=rows * 2 * 10 ** 8, bytes_accessed=rows * 2 ** 19, transcendentals=0),
        name='project',
    )(z_rows, mask_rows, w_t, scale, offset, *after)


def middle_kernel(n_mul, n_mid, n_part, idx_ref, a_ref, *refs):
    b_refs = refs[:n_part]
    zn0_ref, zn1_ref, dy0_ref, dy1_ref, wg_ref, wo_ref, wot_ref, scale_ref, offset_ref = refs[n_part:n_part + 9]
    do0_ref, do1_ref, gl_ref, dwo_ref, dwg_ref, vec_ref, scr = refs[-7:]
    step = pl.program_id(0)
    tile = LANES
    half = tile // 2
    pitch = tile + 1
    chans = wo_ref.shape[0]

    one16 = ones_row(2 * tile)
    one_col = (lax.broadcasted_iota(jnp.int32, (2 * tile, LANES), 1) == 0).astype(F32).astype(BF16)

    @pl.when(step == 0)
    def _():
        dwo_ref[...] = jnp.zeros_like(dwo_ref)
        dwg_ref[...] = jnp.zeros_like(dwg_ref)
        vec_ref[...] = jnp.zeros_like(vec_ref)

    @pl.when(step < n_mul)
    def _():
        for j in range(MID_CH):
            at = (step * MID_CH + j) * pitch
            scr[pl.ds(at, tile), :] = dot_nt(a_ref[j], jnp.concatenate([ref[j] for ref in b_refs], axis=0))

    @pl.when((step >= n_mul) & (step < n_mul + n_mid))
    def _():
        first = (step - n_mul) * MID_ROWS

        def pair(h, carry):
            r0 = first + 2 * h
            tri = jnp.concatenate([scr[pl.ds(r0 + t, chans, stride=pitch), :] for t in range(2)], axis=1)
            centered = tri - col_mean(tri)
            inv_std = lax.rsqrt(col_mean(centered * centered) + LN_EPS)
            o_hat = centered * inv_std
            o_norm = (o_hat * scale_ref[...] + offset_ref[...]).astype(BF16)
            update = dot_nn(wot_ref[...], jnp.concatenate([o_norm, one16], axis=0)).astype(BF16).astype(F32)
            zn = jnp.concatenate([ref[2 * h + t] for t in range(2) for ref in (zn0_ref, zn1_ref)], axis=0)
            sig_g = jax.nn.sigmoid(dot_nt(wg_ref[...], jnp.concatenate([zn, one_col], axis=1)))
            dy_t = jnp.transpose(jnp.concatenate([ref[2 * h + t].astype(F32) for t in range(2) for ref in (dy0_ref, dy1_ref)], axis=0))
            d_update = (sig_g * dy_t).astype(BF16)
            d_gate = dy_t * update * sig_g * (1.0 - sig_g)
            gate16 = d_gate.astype(BF16)
            d_onorm = dot_nn(wo_ref[...], d_update).astype(BF16).astype(F32)
            grad_hat = d_onorm * scale_ref[...]
            d_tri = inv_std * (grad_hat - col_mean(grad_hat) - o_hat * col_mean(grad_hat * o_hat))
            d_upf = d_update.astype(F32)
            d_sc = d_onorm * o_hat
            for t in range(2):
                part = slice(t * tile, (t + 1) * tile)
                scr[pl.ds(r0 + t, chans, stride=pitch), :] = d_tri[:, part]
                gl_ref[2 * h + t] = gate16[:, part]
            vec_ref[0] += d_sc[:, :tile] + d_sc[:, tile:]
            vec_ref[1] += d_onorm[:, :tile] + d_onorm[:, tile:]
            vec_ref[2] += d_upf[:, :tile] + d_upf[:, tile:]
            vec_ref[3] += d_gate[:, :tile] + d_gate[:, tile:]
            dwo_ref[...] += dot_nt(o_norm, d_update)
            dwg_ref[...] += dot_nn(gate16, zn)
            return carry

        lax.fori_loop(0, MID_ROWS // 2, pair, 0)

    @pl.when(step >= n_mul + n_mid)
    def _():
        for j in range(MID_CH):
            at = ((step - n_mul - n_mid) * MID_CH + j) * pitch
            do_t = jnp.transpose(scr[pl.ds(at, tile), :]).astype(BF16)
            do0_ref[j] = do_t[:half]
            do1_ref[j] = do_t[half:]


def middle(pieces, act_a, b_parts, zn, dy_rows, wg_t, wo, wo_t, scale, offset, after=()):
    chans, rows, n_col = act_a.shape
    half = LANES // 2
    n_mul = chans // MID_CH
    n_mid = rows // MID_ROWS
    mul_at = lambda s: jnp.minimum(s, n_mul - 1)
    mid_at = lambda s: jnp.clip(s - n_mul, 0, n_mid - 1)
    out_at = lambda s: jnp.maximum(s - n_mul - n_mid, 0)
    full = lambda shape: pl.BlockSpec(shape, lambda s, q: (0,) * len(shape))
    part_spec = lambda arr: pl.BlockSpec((MID_CH,) + arr.shape[1:], lambda s, q: (mul_at(s), 0, 0))
    piece_spec = lambda n: pl.BlockSpec((MID_ROWS, half, chans), lambda s, q: (mid_at(s), q[n], 0))
    do_spec = pl.BlockSpec((MID_CH, half, rows), lambda s, q: (out_at(s), 0, 0))
    do_type = jax.ShapeDtypeStruct((chans, half, rows), BF16)
    mats = jax.ShapeDtypeStruct((chans, chans), F32)
    return pl.pallas_call(
        functools.partial(middle_kernel, n_mul, n_mid, len(b_parts)),
        grid_spec=pltpu.PrefetchScalarGridSpec(
            num_scalar_prefetch=1,
            grid=(2 * n_mul + n_mid,),
            in_specs=[
                pl.BlockSpec((MID_CH, rows, n_col), lambda s, q: (mul_at(s), 0, 0)),
                *[part_spec(arr) for arr in b_parts],
                piece_spec(0), piece_spec(1), piece_spec(0), piece_spec(1),
                full(wg_t.shape), full(wo.shape), full(wo_t.shape), full(scale.shape), full(offset.shape)]
            + [pl.BlockSpec(memory_space=pl.ANY)] * len(after),
            out_specs=[
                do_spec, do_spec,
                pl.BlockSpec((MID_ROWS, chans, LANES), lambda s, q: (mid_at(s), 0, 0)),
                full((chans, chans)), full((chans, chans)), full((4, chans, LANES))],
            scratch_shapes=[pltpu.VMEM((chans * (LANES + 1), LANES), F32)],
        ),
        out_shape=[
            do_type, do_type,
            jax.ShapeDtypeStruct((rows, chans, LANES), BF16),
            mats, mats, jax.ShapeDtypeStruct((4, chans, LANES), F32)],
        compiler_params=pltpu.CompilerParams(vmem_limit_bytes=VMEM_LIMIT),
        cost_estimate=pl.CostEstimate(flops=25 * 10 ** 9, bytes_accessed=48 * 2 ** 20, transcendentals=0),
        name='middle',
    )(pieces, act_a, *b_parts, zn, zn, dy_rows, dy_rows, wg_t, wo, wo_t, scale, offset, *after)


def grad_kernel(trans, n_do, n_act, n_seed, partial, *refs):
    grads, acts, rest = refs[:n_do], refs[n_do:n_do + n_act], refs[n_do + n_act:]
    step = acts[0].shape[0]
    pitch = step + 1

    def product(c):
        if trans:
            lhs = jnp.concatenate([g[c] for g in grads], axis=0)
        else:
            lhs = jnp.concatenate([jnp.concatenate([g[c] for g in grads[n:n + 2]], axis=1) for n in range(0, n_do, 2)], axis=0)
        rhs = jnp.concatenate([act[c] for act in acts], axis=0)
        acc = dot_tn(lhs, rhs) if trans else dot_nn(lhs, rhs)
        return acc + rest[0][c] if n_seed else acc

    if partial:
        out_ref = rest[-1]

        def block(n, carry):
            for j in range(4):
                out_ref[4 * n + j] = product(4 * n + j)
            return carry

        lax.fori_loop(0, step // 4, block, 0)
        return
    mask_ref, out_ref, scr = rest[n_seed], rest[-2], rest[-1]
    rows, n_col = mask_ref.shape
    plane = rows * pitch

    def block(n, carry):
        for j in range(4):
            acc = product(4 * n + j) * mask_ref[...]
            for t in range(n_col // LANES):
                scr[pl.ds(t * plane + 4 * n + j, rows, stride=pitch), :] = acc[:, t * LANES:(t + 1) * LANES]
        return carry

    lax.fori_loop(0, step // 4, block, 0)

    def pack(i, carry):
        for t in range(n_col // LANES):
            out_ref[i, :, t * LANES:(t + 1) * LANES] = scr[pl.ds(t * plane + i * pitch, step), :].astype(BF16)
        return carry

    lax.fori_loop(0, rows, pack, 0, unroll=8)


def grad_sum(trans, grads, acts, mask_f, part=0, parts=1, seed=None, partial=False, after=()):
    chans = grads[0].shape[0]
    n_col = acts[0].shape[2]
    rows = mask_f.shape[0] // parts
    step = MID_CH
    block = lambda arr: pl.BlockSpec((step,) + arr.shape[1:], lambda s: (s, 0, 0))
    sum_spec = lambda at: pl.BlockSpec((step, rows, n_col), lambda s: (s, at, 0))
    seeds = [] if seed is None else [seed]
    if partial:
        masks, scratch = [], []
        out_spec, out_shape = sum_spec(0), jax.ShapeDtypeStruct((chans, rows, n_col), F32)
    else:
        masks, scratch = [mask_f], [pltpu.VMEM((n_col // LANES * rows * (step + 1), LANES), F32)]
        out_spec = pl.BlockSpec((rows, step, n_col), lambda s: (0, s, 0))
        out_shape = jax.ShapeDtypeStruct((rows, chans, n_col), BF16)
    return pl.pallas_call(
        functools.partial(grad_kernel, trans, len(grads), len(acts), len(seeds), partial),
        grid=(chans // step,),
        in_specs=[block(arr) for arr in list(grads) + list(acts)] + [sum_spec(part)] * len(seeds)
        + [pl.BlockSpec((rows, n_col), lambda s: (part, 0))] * len(masks) + [pl.BlockSpec(memory_space=pl.ANY)] * len(after),
        out_specs=out_spec,
        out_shape=out_shape,
        scratch_shapes=scratch,
        compiler_params=pltpu.CompilerParams(vmem_limit_bytes=VMEM_LIMIT),
        cost_estimate=pl.CostEstimate(flops=12 * 10 ** 9, bytes_accessed=80 * 2 ** 20, transcendentals=0),
    )(*grads, *acts, *seeds, *masks, *after)


def final_kernel(seeded, q_ref, z_ref, dy_ref, da_ref, db_ref, gl0, gl1, gl2, gl3, w_ref, wb_ref, scale_ref, offset_ref, *refs):
    dz_ref, dw_ref, dbin_ref, vec_ref = refs[-4:]
    gls = (gl0, gl1, gl2, gl3)
    chans = z_ref.shape[2]
    n_lane = z_ref.shape[1] // LANES
    side = LANES // 2

    @pl.when(pl.program_id(0) == 0)
    def _():
        if seeded:
            for ref, seed in zip((dw_ref, dbin_ref, vec_ref), refs[:3]):
                ref[...] = seed[...]
        else:
            dw_ref[...] = jnp.zeros_like(dw_ref)
            dbin_ref[...] = jnp.zeros_like(dbin_ref)
            vec_ref[...] = jnp.zeros_like(vec_ref)

    one16 = ones_row(n_lane * LANES)

    def row(i, carry):
        qs = [q_ref[t] for t in range(n_lane)]
        offs = [pl.multiple_of(q * LANES, LANES) for q in qs]
        fold = lambda val: sum(val[:, t * LANES:(t + 1) * LANES] for t in range(n_lane))
        z_rows = jnp.concatenate([z_ref[i, pl.ds(off, LANES), :] for off in offs], axis=0)
        x_hat, inv_std, znt = input_norm(z_rows, scale_ref[...], offset_ref[...])
        proj = dot_nn(w_ref[...], jnp.concatenate([znt, one16], axis=0))
        grad16 = []
        for g in range(chans // GROUP):
            parts = [proj[(4 * g + n) * GROUP:(4 * g + n + 1) * GROUP] for n in range(4)]
            vals = [None] * 4
            for n, ref in enumerate((da_ref, db_ref)):
                grad = jnp.concatenate([ref[i, g * GROUP:(g + 1) * GROUP, pl.ds(off, LANES)] for off in offs], axis=1).astype(F32)
                sig = jax.nn.sigmoid(parts[2 + n])
                vals[n] = grad * sig
                vals[2 + n] = vals[n] * parts[n] * (1.0 - sig)
            for n in range(4):
                dbin_ref[(4 * g + n) * GROUP:(4 * g + n + 1) * GROUP] += fold(vals[n])
                grad16.append(vals[n].astype(BF16))
        grad16 = jnp.concatenate(grad16, axis=0)
        gate = [g[i] for g in gls[:2]] + [g[i][:, part] for part in (slice(0, side), slice(side, LANES)) for g in gls[2:]]
        gate = jnp.concatenate(gate, axis=1)
        dw_ref[...] += dot_nt(znt, grad16)
        d_znorm = dot_nn(wb_ref[...], jnp.concatenate([grad16, gate], axis=0)).astype(BF16).astype(F32)
        vec_ref[0] += fold(d_znorm * x_hat)
        vec_ref[1] += fold(d_znorm)
        grad_hat = d_znorm * scale_ref[...]
        d_in = inv_std * (grad_hat - col_mean(grad_hat) - x_hat * col_mean(grad_hat * x_hat))
        d_rows = jnp.transpose(d_in)
        for t in range(n_lane):
            out = d_rows[t * LANES:(t + 1) * LANES] + dy_ref[i, pl.ds(offs[t], LANES), :].astype(F32)
            dz_ref[i, pl.ds(offs[t], LANES), :] = out.astype(BF16)
        return carry

    lax.fori_loop(0, ROWS, row, 0)


def final(q_all, z_rows, dy_rows, d_a, d_b, gates, w_t, w_back, scale, offset, first, d_z=None, seeds=()):
    _, n_col, chans = z_rows.shape
    n_step = d_b.shape[0] // ROWS
    at = first // ROWS
    full = lambda shape: pl.BlockSpec(shape, lambda s, q: (0,) * len(shape))
    pair_spec = pl.BlockSpec((ROWS, n_col, chans), lambda s, q: (s + at, 0, 0))
    sums = [(chans, 4 * chans), (4 * chans, LANES), (2, chans, LANES)]
    args = [q_all, z_rows, dy_rows, d_a, d_b, *gates, w_t, w_back, scale, offset, *seeds]
    in_specs = ([pair_spec, pair_spec, pl.BlockSpec((ROWS, chans, n_col), lambda s, q: (s + at, 0, 0)),
                 pl.BlockSpec((ROWS, chans, n_col), lambda s, q: (s, 0, 0))]
                + [pl.BlockSpec((ROWS, chans, LANES), lambda s, q: (s + at, 0, 0))] * 4
                + [full(w_t.shape), full(w_back.shape), full(scale.shape), full(offset.shape)]
                + [full(seed.shape) for seed in seeds])
    alias = {}
    if d_z is not None:
        alias = {len(args): 0}
        args.append(d_z)
        in_specs.append(pl.BlockSpec(memory_space=pl.ANY))
    return pl.pallas_call(
        functools.partial(final_kernel, bool(seeds)),
        grid_spec=pltpu.PrefetchScalarGridSpec(
            num_scalar_prefetch=1,
            grid=(n_step,),
            in_specs=in_specs,
            out_specs=[pair_spec] + [full(shape) for shape in sums],
        ),
        out_shape=[jax.ShapeDtypeStruct(z_rows.shape, BF16)] + [jax.ShapeDtypeStruct(shape, F32) for shape in sums],
        input_output_aliases=alias,
        compiler_params=pltpu.CompilerParams(vmem_limit_bytes=VMEM_LIMIT),
        cost_estimate=pl.CostEstimate(flops=30 * 10 ** 9, bytes_accessed=64 * 2 ** 20, transcendentals=0),
        name='final',
    )(*args)


def lane_bcast(vec, width):
    return jnp.broadcast_to(vec.astype(F32)[:, None], (vec.shape[0], width))


def local_step(z_loc, mask_loc, dy_loc, ln_in_scale, ln_in_offset, w_in, b_in, ln_out_scale, ln_out_offset, w_out, b_out, w_gate, b_gate):
    n_dap = lax.axis_size('dap')
    me = lax.axis_index('dap')
    swap = lambda arr, bit: lax.ppermute(arr, 'dap', [(d, d ^ bit) for d in range(n_dap)])
    w_t = with_bias(by_group(w_in).T, by_group(b_in))
    row_sc, row_of = (lane_bcast(v, z_loc.shape[1]) for v in (ln_in_scale, ln_in_offset))
    in_sc, in_of = lane_bcast(ln_in_scale, 256), lane_bcast(ln_in_offset, 256)
    out_sc, out_of = lane_bcast(ln_out_scale, 256), lane_bcast(ln_out_offset, 256)
    z_far = swap(z_loc, 2)
    rows = z_loc.shape[0]
    part = rows // 4
    mask_f = mask_loc.astype(F32)
    mask_loc = mask_loc.reshape(rows, -1, 1, LANES)
    mask_far = swap(mask_loc, 2)
    n_chunk = rows // part
    z_far = []
    for n in range(n_chunk):
        z_from = lax.optimization_barrier(z_loc) if n else z_loc
        z_far.append(swap(z_from[n * part:(n + 1) * part], 2))
    weights = (w_t, in_sc, in_of)
    a_0, b_0, zn = project(z_loc, mask_loc, 0, rows, *weights, True)
    b_1 = swap(b_0, 1)
    a_1 = swap(a_0, 1)
    blocks = [me ^ r for r in range(n_dap)]
    tail = (zn, dy_loc, with_bias(w_gate.T, b_gate), w_out, with_bias(w_out.T, b_out), out_sc, out_of)
    pieces = lambda *vals: jnp.stack(vals).astype(jnp.int32)
    mids = [middle(pieces(2 * blocks[0], 2 * blocks[0] + 1), a_0, [b_0], *tail)]
    mids.append(middle(pieces(2 * blocks[1], 2 * blocks[1] + 1), a_0, [b_1], *tail, after=(mids[0][5],)))
    near_out = [swap(mids[1][0], 1), swap(mids[1][1], 1)]
    a_2, b_2, a_3, b_3, far_out = [], [], [], [], []
    far_b = lambda h: b_2[2 * h:2 * h + 2] + b_3[2 * h:2 * h + 2]
    d_outs = lambda *tiles: [mids[t][n] for t in tiles for n in range(2)]
    order = (mids[1][5],)
    for h in range(2):
        for n in (2 * h, 2 * h + 1):
            a_n, b_n = project(z_far[n], mask_far, n * part, part, *weights, False, after=order)
            b_3.append(swap(b_n, 1))
            a_3.append(swap(a_n, 1))
            a_2.append(a_n)
            b_2.append(b_n)
            order = (a_n,)
            if n == 1:
                part_b = grad_sum(False, [mids[0][0], near_out[0], mids[0][1], near_out[1]], [a_0, a_1], mask_f, partial=True, after=order)
                order = (part_b,)
            if n == 2:
                part_a = grad_sum(True, d_outs(0, 1, 2), [b_0, b_1, *far_b(0)], mask_f, partial=True, after=order)
                order = (part_a,)
        mids.append(middle(pieces(2 * blocks[2] + h, 2 * blocks[3] + h), a_0, far_b(h), *tail, after=order))
        order = (mids[-1][5],)
        far_out.append([swap(mids[2 + h][0], 2), swap(mids[2 + h][1], 3)])
    d_a = grad_sum(True, d_outs(3), far_b(1), mask_f, seed=part_a)
    w_back = jnp.concatenate([by_group(w_in), w_gate], axis=1)
    d_z, seeds = None, ()
    for h in range(2):
        d_b = grad_sum(False, far_out[h], [*a_2, *a_3], mask_f, part=h, parts=2, seed=part_b, after=(d_a,) if h == 0 else (seeds[2],))
        d_z, *seeds = final(jnp.stack(blocks).astype(jnp.int32), z_loc, dy_loc, d_a, d_b, [m[2] for m in mids], w_t, w_back, row_sc, row_of,
                            h * (rows // 2), d_z, seeds)
    dw_t, dbin, vecs = seeds
    d_wo = sum(m[3] for m in mids)
    d_wg = sum(m[4] for m in mids).T
    vec_mid = jnp.sum(sum(m[5] for m in mids), axis=-1)
    vec_in = jnp.sum(vecs, axis=-1)
    summed = lax.psum((vec_in[0], vec_in[1], dw_t, jnp.sum(dbin, axis=-1), vec_mid[0], vec_mid[1], d_wo, vec_mid[2], d_wg, vec_mid[3]), 'dap')
    summed = list(summed)
    summed[2] = from_group(summed[2])
    summed[3] = from_group(summed[3])
    return (d_z,) + tuple(piece.astype(BF16) for piece in summed)


def solution(mesh):
    pair_spec = P(('batch', 'dap'), None, None)
    mask_spec = P(('batch', 'dap'), None)
    vec_rep = P(None)
    mat_rep = P(None, None)
    vec_part = P('batch')
    mat_part = P('batch', None)
    in_specs = (pair_spec, mask_spec, pair_spec, vec_rep, vec_rep, mat_rep, vec_rep, vec_rep, vec_rep, mat_rep, vec_rep, mat_rep, vec_rep)
    out_specs = (pair_spec, vec_part, vec_part, mat_part, vec_part, vec_part, vec_part, mat_part, vec_part, mat_part, vec_part)
    return jax.shard_map(local_step, mesh=mesh, in_specs=in_specs, out_specs=out_specs, check_vma=False)
```

```python
import functools
import jax
import jax.numpy as jnp
from jax import lax
from jax.experimental import pallas as pl
from jax.experimental.pallas import tpu as pltpu
from jax.sharding import PartitionSpec as P

LN_EPS = 1e-5
F32 = jnp.float32
BF16 = jnp.bfloat16
LANES = 128
ROWS = 16
MID_CH = 16
MID_ROWS = 32
GROUP = 16
VMEM_LIMIT = 60 * 1024 * 1024


def col_mean(x_val):
    return jnp.sum(x_val, axis=0, keepdims=True) * (1.0 / x_val.shape[0])


def dot_nn(lhs, rhs):
    return jnp.dot(lhs, rhs, preferred_element_type=F32)


def dot_nt(lhs, rhs):
    return lax.dot_general(lhs, rhs, (((1,), (1,)), ((), ())), preferred_element_type=F32)


def dot_tn(lhs, rhs):
    return lax.dot_general(lhs, rhs, (((0,), (0,)), ((), ())), preferred_element_type=F32)


def input_norm(z_rows, scale, offset):
    z_t = jnp.transpose(z_rows.astype(F32))
    centered = z_t - col_mean(z_t)
    inv_std = lax.rsqrt(col_mean(centered * centered) + LN_EPS)
    x_hat = centered * inv_std
    return x_hat, inv_std, (x_hat * scale + offset).astype(BF16)


def with_bias(mat, vec):
    pad = jnp.zeros((mat.shape[0], LANES - 1), BF16)
    return jnp.concatenate([mat, vec[:, None], pad], axis=1)


def by_group(arr):
    split = arr.reshape(arr.shape[:-1] + (4, -1, GROUP))
    return jnp.swapaxes(split, -3, -2).reshape(arr.shape)


def from_group(arr):
    split = arr.reshape(arr.shape[:-1] + (-1, 4, GROUP))
    return jnp.swapaxes(split, -3, -2).reshape(arr.shape)


def ones_row(width):
    return (lax.broadcasted_iota(jnp.int32, (LANES, width), 0) == 0).astype(F32).astype(BF16)


def project_kernel(keep_norm, z_ref, mask_ref, w_ref, scale_ref, offset_ref, *refs):
    refs = refs[-5:] if keep_norm else refs[-4:]
    a_ref, b_ref = refs[:2]
    scr_a, scr_b = refs[-2:]
    n_lane = z_ref.shape[1] // LANES
    chans = z_ref.shape[2]
    pitch = ROWS + 1
    plane = chans * pitch
    one16 = ones_row(256)

    def row(i, carry):
        for half in range(n_lane // 2):
            cols = slice(half * 256, half * 256 + 256)
            _, _, znt = input_norm(z_ref[i, cols, :], scale_ref[...], offset_ref[...])
            if keep_norm:
                refs[2][i, cols, :] = jnp.transpose(znt)
            mask16 = jnp.concatenate([mask_ref[i, half * 2 + t] for t in range(2)], axis=1).astype(F32).astype(BF16)
            proj = dot_nn(w_ref[...], jnp.concatenate([znt * mask16, one16 * mask16], axis=0))
            for g in range(chans // GROUP):
                pa, pb, la, lb = [proj[(4 * g + n) * GROUP:(4 * g + n + 1) * GROUP] for n in range(4)]
                for scr, val in ((scr_a, jax.nn.sigmoid(la) * pa), (scr_b, jax.nn.sigmoid(lb) * pb)):
                    for t in range(2):
                        at = (half * 2 + t) * plane + g * GROUP * pitch + i
                        scr[pl.ds(at, GROUP, stride=pitch), :] = val[:, t * LANES:(t + 1) * LANES]
        return carry

    lax.fori_loop(0, ROWS, row, 0, unroll=2)

    def pack(c, carry):
        for t in range(n_lane):
            lanes = slice(t * LANES, (t + 1) * LANES)
            at = t * plane + c * pitch
            a_ref[c, :, lanes] = scr_a[pl.ds(at, ROWS), :].astype(BF16)
            b_ref[c, :, lanes] = scr_b[pl.ds(at, ROWS), :].astype(BF16)
        return carry

    lax.fori_loop(0, chans, pack, 0, unroll=4)


def project(z_rows, mask_rows, first, rows, w_t, scale, offset, keep_norm, after=()):
    _, n_col, chans = z_rows.shape
    z_from, m_from = (0 if z_rows.shape[0] == rows else first // ROWS), first // ROWS
    full = lambda arr: pl.BlockSpec(arr.shape, lambda s: (0,) * arr.ndim)
    act = jax.ShapeDtypeStruct((chans, rows, n_col), BF16)
    act_spec = pl.BlockSpec((chans, ROWS, n_col), lambda s: (0, s, 0))
    out_shape = [act, act]
    out_specs = [act_spec, act_spec]
    pair_spec = pl.BlockSpec((ROWS, n_col, chans), lambda s: (s + z_from, 0, 0))
    if keep_norm:
        out_shape.append(jax.ShapeDtypeStruct((rows, n_col, chans), BF16))
        out_specs.append(pair_spec)
    scratch = pltpu.VMEM((n_col // LANES * chans * (ROWS + 1), LANES), F32)
    return pl.pallas_call(
        functools.partial(project_kernel, keep_norm),
        grid=(rows // ROWS,),
        in_specs=[
            pair_spec,
            pl.BlockSpec((ROWS,) + mask_rows.shape[1:], lambda s: (s + m_from, 0, 0, 0)),
            full(w_t), full(scale), full(offset)] + [pl.BlockSpec(memory_space=pl.ANY)] * len(after),
        out_specs=out_specs,
        out_shape=out_shape,
        scratch_shapes=[scratch, scratch],
        compiler_params=pltpu.CompilerParams(vmem_limit_bytes=VMEM_LIMIT),
        cost_estimate=pl.CostEstimate(flops=rows * 2 * 10 ** 8, bytes_accessed=rows * 2 ** 19, transcendentals=0),
        name='project',
    )(z_rows, mask_rows, w_t, scale, offset, *after)


def middle_kernel(n_mul, n_mid, n_part, idx_ref, a_ref, *refs):
    b_refs = refs[:n_part]
    zn0_ref, zn1_ref, dy0_ref, dy1_ref, wg_ref, wo_ref, wot_ref, scale_ref, offset_ref = refs[n_part:n_part + 9]
    do0_ref, do1_ref, gl_ref, dwo_ref, dwg_ref, vec_ref, scr = refs[-7:]
    step = pl.program_id(0)
    tile = LANES
    half = tile // 2
    pitch = tile + 1
    chans = wo_ref.shape[0]

    one16 = ones_row(2 * tile)
    one_col = (lax.broadcasted_iota(jnp.int32, (2 * tile, LANES), 1) == 0).astype(F32).astype(BF16)

    @pl.when(step == 0)
    def _():
        dwo_ref[...] = jnp.zeros_like(dwo_ref)
        dwg_ref[...] = jnp.zeros_like(dwg_ref)
        vec_ref[...] = jnp.zeros_like(vec_ref)

    @pl.when(step < n_mul)
    def _():
        for j in range(MID_CH):
            at = (step * MID_CH + j) * pitch
            scr[pl.ds(at, tile), :] = dot_nt(a_ref[j], jnp.concatenate([ref[j] for ref in b_refs], axis=0))

    @pl.when((step >= n_mul) & (step < n_mul + n_mid))
    def _():
        first = (step - n_mul) * MID_ROWS

        def pair(h, carry):
            r0 = first + 2 * h
            tri = jnp.concatenate([scr[pl.ds(r0 + t, chans, stride=pitch), :] for t in range(2)], axis=1)
            centered = tri - col_mean(tri)
            inv_std = lax.rsqrt(col_mean(centered * centered) + LN_EPS)
            o_hat = centered * inv_std
            o_norm = (o_hat * scale_ref[...] + offset_ref[...]).astype(BF16)
            update = dot_nn(wot_ref[...], jnp.concatenate([o_norm, one16], axis=0)).astype(BF16).astype(F32)
            zn = jnp.concatenate([ref[2 * h + t] for t in range(2) for ref in (zn0_ref, zn1_ref)], axis=0)
            sig_g = jax.nn.sigmoid(dot_nt(wg_ref[...], jnp.concatenate([zn, one_col], axis=1)))
            dy_t = jnp.transpose(jnp.concatenate([ref[2 * h + t].astype(F32) for t in range(2) for ref in (dy0_ref, dy1_ref)], axis=0))
            d_update = (sig_g * dy_t).astype(BF16)
            d_gate = dy_t * update * sig_g * (1.0 - sig_g)
            gate16 = d_gate.astype(BF16)
            d_onorm = dot_nn(wo_ref[...], d_update).astype(BF16).astype(F32)
            grad_hat = d_onorm * scale_ref[...]
            d_tri = inv_std * (grad_hat - col_mean(grad_hat) - o_hat * col_mean(grad_hat * o_hat))
            d_upf = d_update.astype(F32)
            d_sc = d_onorm * o_hat
            for t in range(2):
                part = slice(t * tile, (t + 1) * tile)
                scr[pl.ds(r0 + t, chans, stride=pitch), :] = d_tri[:, part]
                gl_ref[2 * h + t] = gate16[:, part]
            vec_ref[0] += d_sc[:, :tile] + d_sc[:, tile:]
            vec_ref[1] += d_onorm[:, :tile] + d_onorm[:, tile:]
            vec_ref[2] += d_upf[:, :tile] + d_upf[:, tile:]
            vec_ref[3] += d_gate[:, :tile] + d_gate[:, tile:]
            dwo_ref[...] += dot_nt(o_norm, d_update)
            dwg_ref[...] += dot_nn(gate16, zn)
            return carry

        lax.fori_loop(0, MID_ROWS // 2, pair, 0, unroll=2)

    @pl.when(step >= n_mul + n_mid)
    def _():
        for j in range(MID_CH):
            at = ((step - n_mul - n_mid) * MID_CH + j) * pitch
            do_t = jnp.transpose(scr[pl.ds(at, tile), :]).astype(BF16)
            do0_ref[j] = do_t[:half]
            do1_ref[j] = do_t[half:]


def middle(pieces, act_a, b_parts, zn, dy_rows, wg_t, wo, wo_t, scale, offset, after=()):
    chans, rows, n_col = act_a.shape
    half = LANES // 2
    n_mul = chans // MID_CH
    n_mid = rows // MID_ROWS
    mul_at = lambda s: jnp.minimum(s, n_mul - 1)
    mid_at = lambda s: jnp.clip(s - n_mul, 0, n_mid - 1)
    out_at = lambda s: jnp.maximum(s - n_mul - n_mid, 0)
    full = lambda shape: pl.BlockSpec(shape, lambda s, q: (0,) * len(shape))
    part_spec = lambda arr: pl.BlockSpec((MID_CH,) + arr.shape[1:], lambda s, q: (mul_at(s), 0, 0))
    piece_spec = lambda n: pl.BlockSpec((MID_ROWS, half, chans), lambda s, q: (mid_at(s), q[n], 0))
    do_spec = pl.BlockSpec((MID_CH, half, rows), lambda s, q: (out_at(s), 0, 0))
    do_type = jax.ShapeDtypeStruct((chans, half, rows), BF16)
    mats = jax.ShapeDtypeStruct((chans, chans), F32)
    return pl.pallas_call(
        functools.partial(middle_kernel, n_mul, n_mid, len(b_parts)),
        grid_spec=pltpu.PrefetchScalarGridSpec(
            num_scalar_prefetch=1,
            grid=(2 * n_mul + n_mid,),
            in_specs=[
                pl.BlockSpec((MID_CH, rows, n_col), lambda s, q: (mul_at(s), 0, 0)),
                *[part_spec(arr) for arr in b_parts],
                piece_spec(0), piece_spec(1), piece_spec(0), piece_spec(1),
                full(wg_t.shape), full(wo.shape), full(wo_t.shape), full(scale.shape), full(offset.shape)]
            + [pl.BlockSpec(memory_space=pl.ANY)] * len(after),
            out_specs=[
                do_spec, do_spec,
                pl.BlockSpec((MID_ROWS, chans, LANES), lambda s, q: (mid_at(s), 0, 0)),
                full((chans, chans)), full((chans, chans)), full((4, chans, LANES))],
            scratch_shapes=[pltpu.VMEM((chans * (LANES + 1), LANES), F32)],
        ),
        out_shape=[
            do_type, do_type,
            jax.ShapeDtypeStruct((rows, chans, LANES), BF16),
            mats, mats, jax.ShapeDtypeStruct((4, chans, LANES), F32)],
        compiler_params=pltpu.CompilerParams(vmem_limit_bytes=VMEM_LIMIT),
        cost_estimate=pl.CostEstimate(flops=25 * 10 ** 9, bytes_accessed=48 * 2 ** 20, transcendentals=0),
        name='middle',
    )(pieces, act_a, *b_parts, zn, zn, dy_rows, dy_rows, wg_t, wo, wo_t, scale, offset, *after)


def grad_kernel(trans, n_do, n_act, n_seed, partial, *refs):
    grads, acts, rest = refs[:n_do], refs[n_do:n_do + n_act], refs[n_do + n_act:]
    step = acts[0].shape[0]
    pitch = step + 1

    def product(c):
        if trans:
            lhs = jnp.concatenate([g[c] for g in grads], axis=0)
        else:
            lhs = jnp.concatenate([jnp.concatenate([g[c] for g in grads[n:n + 2]], axis=1) for n in range(0, n_do, 2)], axis=0)
        rhs = jnp.concatenate([act[c] for act in acts], axis=0)
        acc = dot_tn(lhs, rhs) if trans else dot_nn(lhs, rhs)
        return acc + rest[0][c] if n_seed else acc

    if partial:
        out_ref = rest[-1]

        def block(n, carry):
            for j in range(4):
                out_ref[4 * n + j] = product(4 * n + j)
            return carry

        lax.fori_loop(0, step // 4, block, 0)
        return
    mask_ref, out_ref, scr = rest[n_seed], rest[-2], rest[-1]
    rows, n_col = mask_ref.shape
    plane = rows * pitch

    def block(n, carry):
        for j in range(4):
            acc = product(4 * n + j) * mask_ref[...]
            for t in range(n_col // LANES):
                scr[pl.ds(t * plane + 4 * n + j, rows, stride=pitch), :] = acc[:, t * LANES:(t + 1) * LANES]
        return carry

    lax.fori_loop(0, step // 4, block, 0)

    def pack(i, carry):
        for t in range(n_col // LANES):
            out_ref[i, :, t * LANES:(t + 1) * LANES] = scr[pl.ds(t * plane + i * pitch, step), :].astype(BF16)
        return carry

    lax.fori_loop(0, rows, pack, 0, unroll=8)


def grad_sum(trans, grads, acts, mask_f, part=0, parts=1, seed=None, partial=False, after=()):
    chans = grads[0].shape[0]
    n_col = acts[0].shape[2]
    rows = mask_f.shape[0] // parts
    step = MID_CH
    block = lambda arr: pl.BlockSpec((step,) + arr.shape[1:], lambda s: (s, 0, 0))
    sum_spec = lambda at: pl.BlockSpec((step, rows, n_col), lambda s: (s, at, 0))
    seeds = [] if seed is None else [seed]
    if partial:
        masks, scratch = [], []
        out_spec, out_shape = sum_spec(0), jax.ShapeDtypeStruct((chans, rows, n_col), F32)
    else:
        masks, scratch = [mask_f], [pltpu.VMEM((n_col // LANES * rows * (step + 1), LANES), F32)]
        out_spec = pl.BlockSpec((rows, step, n_col), lambda s: (0, s, 0))
        out_shape = jax.ShapeDtypeStruct((rows, chans, n_col), BF16)
    return pl.pallas_call(
        functools.partial(grad_kernel, trans, len(grads), len(acts), len(seeds), partial),
        grid=(chans // step,),
        in_specs=[block(arr) for arr in list(grads) + list(acts)] + [sum_spec(part)] * len(seeds)
        + [pl.BlockSpec((rows, n_col), lambda s: (part, 0))] * len(masks) + [pl.BlockSpec(memory_space=pl.ANY)] * len(after),
        out_specs=out_spec,
        out_shape=out_shape,
        scratch_shapes=scratch,
        compiler_params=pltpu.CompilerParams(vmem_limit_bytes=VMEM_LIMIT),
        cost_estimate=pl.CostEstimate(flops=12 * 10 ** 9, bytes_accessed=80 * 2 ** 20, transcendentals=0),
    )(*grads, *acts, *seeds, *masks, *after)


def final_kernel(seeded, q_ref, z_ref, dy_ref, da_ref, db_ref, gl0, gl1, gl2, gl3, w_ref, wb_ref, scale_ref, offset_ref, *refs):
    dz_ref, dw_ref, dbin_ref, vec_ref = refs[-4:]
    gls = (gl0, gl1, gl2, gl3)
    chans = z_ref.shape[2]
    n_lane = z_ref.shape[1] // LANES
    side = LANES // 2

    @pl.when(pl.program_id(0) == 0)
    def _():
        if seeded:
            for ref, seed in zip((dw_ref, dbin_ref, vec_ref), refs[:3]):
                ref[...] = seed[...]
        else:
            dw_ref[...] = jnp.zeros_like(dw_ref)
            dbin_ref[...] = jnp.zeros_like(dbin_ref)
            vec_ref[...] = jnp.zeros_like(vec_ref)

    one16 = ones_row(n_lane * LANES)

    def row(i, carry):
        qs = [q_ref[t] for t in range(n_lane)]
        offs = [pl.multiple_of(q * LANES, LANES) for q in qs]
        fold = lambda val: sum(val[:, t * LANES:(t + 1) * LANES] for t in range(n_lane))
        z_rows = jnp.concatenate([z_ref[i, pl.ds(off, LANES), :] for off in offs], axis=0)
        x_hat, inv_std, znt = input_norm(z_rows, scale_ref[...], offset_ref[...])
        proj = dot_nn(w_ref[...], jnp.concatenate([znt, one16], axis=0))
        grad16 = []
        for g in range(chans // GROUP):
            parts = [proj[(4 * g + n) * GROUP:(4 * g + n + 1) * GROUP] for n in range(4)]
            vals = [None] * 4
            for n, ref in enumerate((da_ref, db_ref)):
                grad = jnp.concatenate([ref[i, g * GROUP:(g + 1) * GROUP, pl.ds(off, LANES)] for off in offs], axis=1).astype(F32)
                sig = jax.nn.sigmoid(parts[2 + n])
                vals[n] = grad * sig
                vals[2 + n] = vals[n] * parts[n] * (1.0 - sig)
            for n in range(4):
                dbin_ref[(4 * g + n) * GROUP:(4 * g + n + 1) * GROUP] += fold(vals[n])
                grad16.append(vals[n].astype(BF16))
        grad16 = jnp.concatenate(grad16, axis=0)
        gate = [g[i] for g in gls[:2]] + [g[i][:, part] for part in (slice(0, side), slice(side, LANES)) for g in gls[2:]]
        gate = jnp.concatenate(gate, axis=1)
        dw_ref[...] += dot_nn(grad16, jnp.transpose(znt))
        d_znorm = dot_nn(wb_ref[...], jnp.concatenate([grad16, gate], axis=0)).astype(BF16).astype(F32)
        vec_ref[0] += fold(d_znorm * x_hat)
        vec_ref[1] += fold(d_znorm)
        grad_hat = d_znorm * scale_ref[...]
        d_in = inv_std * (grad_hat - col_mean(grad_hat) - x_hat * col_mean(grad_hat * x_hat))
        d_rows = jnp.transpose(d_in)
        for t in range(n_lane):
            out = d_rows[t * LANES:(t + 1) * LANES] + dy_ref[i, pl.ds(offs[t], LANES), :].astype(F32)
            dz_ref[i, pl.ds(offs[t], LANES), :] = out.astype(BF16)
        return carry

    lax.fori_loop(0, ROWS, row, 0, unroll=2)


def final(q_all, z_rows, dy_rows, d_a, d_b, gates, w_t, w_back, scale, offset, first, d_z=None, seeds=()):
    _, n_col, chans = z_rows.shape
    n_step = d_b.shape[0] // ROWS
    at = first // ROWS
    full = lambda shape: pl.BlockSpec(shape, lambda s, q: (0,) * len(shape))
    pair_spec = pl.BlockSpec((ROWS, n_col, chans), lambda s, q: (s + at, 0, 0))
    sums = [(4 * chans, chans), (4 * chans, LANES), (2, chans, LANES)]
    args = [q_all, z_rows, dy_rows, d_a, d_b, *gates, w_t, w_back, scale, offset, *seeds]
    in_specs = ([pair_spec, pair_spec, pl.BlockSpec((ROWS, chans, n_col), lambda s, q: (s + at, 0, 0)),
                 pl.BlockSpec((ROWS, chans, n_col), lambda s, q: (s, 0, 0))]
                + [pl.BlockSpec((ROWS, chans, LANES), lambda s, q: (s + at, 0, 0))] * 4
                + [full(w_t.shape), full(w_back.shape), full(scale.shape), full(offset.shape)]
                + [full(seed.shape) for seed in seeds])
    alias = {}
    if d_z is not None:
        alias = {len(args): 0}
        args.append(d_z)
        in_specs.append(pl.BlockSpec(memory_space=pl.ANY))
    return pl.pallas_call(
        functools.partial(final_kernel, bool(seeds)),
        grid_spec=pltpu.PrefetchScalarGridSpec(
            num_scalar_prefetch=1,
            grid=(n_step,),
            in_specs=in_specs,
            out_specs=[pair_spec] + [full(shape) for shape in sums],
        ),
        out_shape=[jax.ShapeDtypeStruct(z_rows.shape, BF16)] + [jax.ShapeDtypeStruct(shape, F32) for shape in sums],
        input_output_aliases=alias,
        compiler_params=pltpu.CompilerParams(vmem_limit_bytes=VMEM_LIMIT),
        cost_estimate=pl.CostEstimate(flops=30 * 10 ** 9, bytes_accessed=64 * 2 ** 20, transcendentals=0),
        name='final',
    )(*args)


def lane_bcast(vec, width):
    return jnp.broadcast_to(vec.astype(F32)[:, None], (vec.shape[0], width))


def local_step(z_loc, mask_loc, dy_loc, ln_in_scale, ln_in_offset, w_in, b_in, ln_out_scale, ln_out_offset, w_out, b_out, w_gate, b_gate):
    n_dap = lax.axis_size('dap')
    me = lax.axis_index('dap')
    swap = lambda arr, bit: lax.ppermute(arr, 'dap', [(d, d ^ bit) for d in range(n_dap)])
    w_t = with_bias(by_group(w_in).T, by_group(b_in))
    row_sc, row_of = (lane_bcast(v, z_loc.shape[1]) for v in (ln_in_scale, ln_in_offset))
    in_sc, in_of = lane_bcast(ln_in_scale, 256), lane_bcast(ln_in_offset, 256)
    out_sc, out_of = lane_bcast(ln_out_scale, 256), lane_bcast(ln_out_offset, 256)
    z_far = swap(z_loc, 2)
    rows = z_loc.shape[0]
    part = rows // 4
    mask_f = mask_loc.astype(F32)
    mask_loc = mask_loc.reshape(rows, -1, 1, LANES)
    mask_far = swap(mask_loc, 2)
    n_chunk = rows // part
    z_far = []
    for n in range(n_chunk):
        z_from = lax.optimization_barrier(z_loc) if n else z_loc
        z_far.append(swap(z_from[n * part:(n + 1) * part], 2))
    weights = (w_t, in_sc, in_of)
    a_0, b_0, zn = project(z_loc, mask_loc, 0, rows, *weights, True)
    b_1 = swap(b_0, 1)
    a_1 = swap(a_0, 1)
    blocks = [me ^ r for r in range(n_dap)]
    tail = (zn, dy_loc, with_bias(w_gate.T, b_gate), w_out, with_bias(w_out.T, b_out), out_sc, out_of)
    pieces = lambda *vals: jnp.stack(vals).astype(jnp.int32)
    mids = [middle(pieces(2 * blocks[0], 2 * blocks[0] + 1), a_0, [b_0], *tail)]
    mids.append(middle(pieces(2 * blocks[1], 2 * blocks[1] + 1), a_0, [b_1], *tail, after=(mids[0][5],)))
    near_out = [swap(mids[1][0], 1), swap(mids[1][1], 1)]
    a_2, b_2, a_3, b_3, far_out = [], [], [], [], []
    far_b = lambda h: b_2[2 * h:2 * h + 2] + b_3[2 * h:2 * h + 2]
    d_outs = lambda *tiles: [mids[t][n] for t in tiles for n in range(2)]
    order = (mids[1][5],)
    for h in range(2):
        for n in (2 * h, 2 * h + 1):
            a_n, b_n = project(z_far[n], mask_far, n * part, part, *weights, False, after=order)
            b_3.append(swap(b_n, 1))
            a_3.append(swap(a_n, 1))
            a_2.append(a_n)
            b_2.append(b_n)
            order = (a_n,)
            if n == 1:
                part_b = grad_sum(False, [mids[0][0], near_out[0], mids[0][1], near_out[1]], [a_0, a_1], mask_f, partial=True, after=order)
                order = (part_b,)
            if n == 2:
                part_a = grad_sum(True, d_outs(0, 1, 2), [b_0, b_1, *far_b(0)], mask_f, partial=True, after=order)
                order = (part_a,)
        mids.append(middle(pieces(2 * blocks[2] + h, 2 * blocks[3] + h), a_0, far_b(h), *tail, after=order))
        order = (mids[-1][5],)
        far_out.append([swap(mids[2 + h][0], 2), swap(mids[2 + h][1], 3)])
    d_a = grad_sum(True, d_outs(3), far_b(1), mask_f, seed=part_a)
    w_back = jnp.concatenate([by_group(w_in), w_gate], axis=1)
    d_z, seeds = None, ()
    for h in range(2):
        d_b = grad_sum(False, far_out[h], [*a_2, *a_3], mask_f, part=h, parts=2, seed=part_b, after=(d_a,) if h == 0 else (seeds[2],))
        d_z, *seeds = final(jnp.stack(blocks).astype(jnp.int32), z_loc, dy_loc, d_a, d_b, [m[2] for m in mids], w_t, w_back, row_sc, row_of,
                            h * (rows // 2), d_z, seeds)
    dw_t, dbin, vecs = seeds
    d_wo = sum(m[3] for m in mids)
    d_wg = sum(m[4] for m in mids).T
    vec_mid = jnp.sum(sum(m[5] for m in mids), axis=-1)
    vec_in = jnp.sum(vecs, axis=-1)
    summed = lax.psum((vec_in[0], vec_in[1], dw_t, jnp.sum(dbin, axis=-1), vec_mid[0], vec_mid[1], d_wo, vec_mid[2], d_wg, vec_mid[3]), 'dap')
    summed = list(summed)
    summed[2] = from_group(summed[2].T)
    summed[3] = from_group(summed[3])
    return (d_z,) + tuple(piece.astype(BF16) for piece in summed)


def solution(mesh):
    pair_spec = P(('batch', 'dap'), None, None)
    mask_spec = P(('batch', 'dap'), None)
    vec_rep = P(None)
    mat_rep = P(None, None)
    vec_part = P('batch')
    mat_part = P('batch', None)
    in_specs = (pair_spec, mask_spec, pair_spec, vec_rep, vec_rep, mat_rep, vec_rep, vec_rep, vec_rep, mat_rep, vec_rep, mat_rep, vec_rep)
    out_specs = (pair_spec, vec_part, vec_part, mat_part, vec_part, vec_part, vec_part, mat_part, vec_part, mat_part, vec_part)
    return jax.shard_map(local_step, mesh=mesh, in_specs=in_specs, out_specs=out_specs, check_vma=False)
```

```python
import functools
import jax
import jax.numpy as jnp
from jax import lax
from jax.experimental import pallas as pl
from jax.experimental.pallas import tpu as pltpu
from jax.sharding import PartitionSpec as P

LN_EPS = 1e-5
F32 = jnp.float32
BF16 = jnp.bfloat16
LANES = 128
ROWS = 16
MID_CH = 16
MID_ROWS = 32
GROUP = 16
VMEM_LIMIT = 60 * 1024 * 1024


def col_mean(x_val):
    return jnp.sum(x_val, axis=0, keepdims=True) * (1.0 / x_val.shape[0])


def dot_nn(lhs, rhs):
    return jnp.dot(lhs, rhs, preferred_element_type=F32)


def dot_nt(lhs, rhs):
    return lax.dot_general(lhs, rhs, (((1,), (1,)), ((), ())), preferred_element_type=F32)


def dot_tn(lhs, rhs):
    return lax.dot_general(lhs, rhs, (((0,), (0,)), ((), ())), preferred_element_type=F32)


def input_norm(z_rows, scale, offset):
    z_t = jnp.transpose(z_rows.astype(F32))
    centered = z_t - col_mean(z_t)
    inv_std = lax.rsqrt(col_mean(centered * centered) + LN_EPS)
    x_hat = centered * inv_std
    return x_hat, inv_std, (x_hat * scale + offset).astype(BF16)


def with_bias(mat, vec):
    pad = jnp.zeros((mat.shape[0], LANES - 1), BF16)
    return jnp.concatenate([mat, vec[:, None], pad], axis=1)


def by_group(arr):
    split = arr.reshape(arr.shape[:-1] + (4, -1, GROUP))
    return jnp.swapaxes(split, -3, -2).reshape(arr.shape)


def from_group(arr):
    split = arr.reshape(arr.shape[:-1] + (-1, 4, GROUP))
    return jnp.swapaxes(split, -3, -2).reshape(arr.shape)


def ones_row(width):
    return (lax.broadcasted_iota(jnp.int32, (LANES, width), 0) == 0).astype(F32).astype(BF16)


def project_kernel(keep_norm, z_ref, mask_ref, w_ref, scale_ref, offset_ref, *refs):
    refs = refs[-5:] if keep_norm else refs[-4:]
    a_ref, b_ref = refs[:2]
    scr_a, scr_b = refs[-2:]
    n_lane = z_ref.shape[1] // LANES
    chans = z_ref.shape[2]
    pitch = ROWS + 1
    plane = chans * pitch
    one16 = ones_row(256)

    def row(i, carry):
        for half in range(n_lane // 2):
            cols = slice(half * 256, half * 256 + 256)
            _, _, znt = input_norm(z_ref[i, cols, :], scale_ref[...], offset_ref[...])
            if keep_norm:
                refs[2][i, cols, :] = jnp.transpose(znt)
            mask16 = jnp.concatenate([mask_ref[i, half * 2 + t] for t in range(2)], axis=1).astype(F32).astype(BF16)
            proj = dot_nn(w_ref[...], jnp.concatenate([znt * mask16, one16 * mask16], axis=0))
            for g in range(chans // GROUP):
                pa, pb, la, lb = [proj[(4 * g + n) * GROUP:(4 * g + n + 1) * GROUP] for n in range(4)]
                for scr, val in ((scr_a, jax.nn.sigmoid(la) * pa), (scr_b, jax.nn.sigmoid(lb) * pb)):
                    for t in range(2):
                        at = (half * 2 + t) * plane + g * GROUP * pitch + i
                        scr[pl.ds(at, GROUP, stride=pitch), :] = val[:, t * LANES:(t + 1) * LANES]
        return carry

    lax.fori_loop(0, ROWS, row, 0, unroll=4)

    def pack(c, carry):
        for t in range(n_lane):
            lanes = slice(t * LANES, (t + 1) * LANES)
            at = t * plane + c * pitch
            a_ref[c, :, lanes] = scr_a[pl.ds(at, ROWS), :].astype(BF16)
            b_ref[c, :, lanes] = scr_b[pl.ds(at, ROWS), :].astype(BF16)
        return carry

    lax.fori_loop(0, chans, pack, 0, unroll=4)


def project(z_rows, mask_rows, first, rows, w_t, scale, offset, keep_norm, after=()):
    _, n_col, chans = z_rows.shape
    z_from, m_from = (0 if z_rows.shape[0] == rows else first // ROWS), first // ROWS
    full = lambda arr: pl.BlockSpec(arr.shape, lambda s: (0,) * arr.ndim)
    act = jax.ShapeDtypeStruct((chans, rows, n_col), BF16)
    act_spec = pl.BlockSpec((chans, ROWS, n_col), lambda s: (0, s, 0))
    out_shape = [act, act]
    out_specs = [act_spec, act_spec]
    pair_spec = pl.BlockSpec((ROWS, n_col, chans), lambda s: (s + z_from, 0, 0))
    if keep_norm:
        out_shape.append(jax.ShapeDtypeStruct((rows, n_col, chans), BF16))
        out_specs.append(pair_spec)
    scratch = pltpu.VMEM((n_col // LANES * chans * (ROWS + 1), LANES), F32)
    return pl.pallas_call(
        functools.partial(project_kernel, keep_norm),
        grid=(rows // ROWS,),
        in_specs=[
            pair_spec,
            pl.BlockSpec((ROWS,) + mask_rows.shape[1:], lambda s: (s + m_from, 0, 0, 0)),
            full(w_t), full(scale), full(offset)] + [pl.BlockSpec(memory_space=pl.ANY)] * len(after),
        out_specs=out_specs,
        out_shape=out_shape,
        scratch_shapes=[scratch, scratch],
        compiler_params=pltpu.CompilerParams(vmem_limit_bytes=VMEM_LIMIT),
        cost_estimate=pl.CostEstimate(flops=rows * 2 * 10 ** 8, bytes_accessed=rows * 2 ** 19, transcendentals=0),
        name='project',
    )(z_rows, mask_rows, w_t, scale, offset, *after)


def middle_kernel(n_mul, n_mid, n_part, idx_ref, a_ref, *refs):
    b_refs = refs[:n_part]
    zn0_ref, zn1_ref, dy0_ref, dy1_ref, wg_ref, wo_ref, wot_ref, scale_ref, offset_ref = refs[n_part:n_part + 9]
    do0_ref, do1_ref, gl_ref, dwo_ref, dwg_ref, vec_ref, scr = refs[-7:]
    step = pl.program_id(0)
    tile = LANES
    half = tile // 2
    pitch = tile + 1
    chans = wo_ref.shape[0]

    one16 = ones_row(2 * tile)
    one_col = (lax.broadcasted_iota(jnp.int32, (2 * tile, LANES), 1) == 0).astype(F32).astype(BF16)

    @pl.when(step == 0)
    def _():
        dwo_ref[...] = jnp.zeros_like(dwo_ref)
        dwg_ref[...] = jnp.zeros_like(dwg_ref)
        vec_ref[...] = jnp.zeros_like(vec_ref)

    @pl.when(step < n_mul)
    def _():
        for j in range(MID_CH):
            at = (step * MID_CH + j) * pitch
            scr[pl.ds(at, tile), :] = dot_nt(a_ref[j], jnp.concatenate([ref[j] for ref in b_refs], axis=0))

    @pl.when((step >= n_mul) & (step < n_mul + n_mid))
    def _():
        first = (step - n_mul) * MID_ROWS

        def pair(h, carry):
            r0 = first + 2 * h
            tri = jnp.concatenate([scr[pl.ds(r0 + t, chans, stride=pitch), :] for t in range(2)], axis=1)
            centered = tri - col_mean(tri)
            inv_std = lax.rsqrt(col_mean(centered * centered) + LN_EPS)
            o_hat = centered * inv_std
            o_norm = (o_hat * scale_ref[...] + offset_ref[...]).astype(BF16)
            update = dot_nn(wot_ref[...], jnp.concatenate([o_norm, one16], axis=0)).astype(BF16).astype(F32)
            zn = jnp.concatenate([ref[2 * h + t] for t in range(2) for ref in (zn0_ref, zn1_ref)], axis=0)
            sig_g = jax.nn.sigmoid(dot_nt(wg_ref[...], jnp.concatenate([zn, one_col], axis=1)))
            dy_t = jnp.transpose(jnp.concatenate([ref[2 * h + t].astype(F32) for t in range(2) for ref in (dy0_ref, dy1_ref)], axis=0))
            d_update = (sig_g * dy_t).astype(BF16)
            d_gate = dy_t * update * sig_g * (1.0 - sig_g)
            gate16 = d_gate.astype(BF16)
            d_onorm = dot_nn(wo_ref[...], d_update).astype(BF16).astype(F32)
            grad_hat = d_onorm * scale_ref[...]
            d_tri = inv_std * (grad_hat - col_mean(grad_hat) - o_hat * col_mean(grad_hat * o_hat))
            d_upf = d_update.astype(F32)
            d_sc = d_onorm * o_hat
            for t in range(2):
                part = slice(t * tile, (t + 1) * tile)
                scr[pl.ds(r0 + t, chans, stride=pitch), :] = d_tri[:, part]
                gl_ref[2 * h + t] = gate16[:, part]
            vec_ref[0] += d_sc[:, :tile] + d_sc[:, tile:]
            vec_ref[1] += d_onorm[:, :tile] + d_onorm[:, tile:]
            vec_ref[2] += d_upf[:, :tile] + d_upf[:, tile:]
            vec_ref[3] += d_gate[:, :tile] + d_gate[:, tile:]
            dwo_ref[...] += dot_nt(o_norm, d_update)
            dwg_ref[...] += dot_nn(gate16, zn)
            return carry

        lax.fori_loop(0, MID_ROWS // 2, pair, 0, unroll=4)

    @pl.when(step >= n_mul + n_mid)
    def _():
        for j in range(MID_CH):
            at = ((step - n_mul - n_mid) * MID_CH + j) * pitch
            do_t = jnp.transpose(scr[pl.ds(at, tile), :]).astype(BF16)
            do0_ref[j] = do_t[:half]
            do1_ref[j] = do_t[half:]


def middle(pieces, act_a, b_parts, zn, dy_rows, wg_t, wo, wo_t, scale, offset, after=()):
    chans, rows, n_col = act_a.shape
    half = LANES // 2
    n_mul = chans // MID_CH
    n_mid = rows // MID_ROWS
    mul_at = lambda s: jnp.minimum(s, n_mul - 1)
    mid_at = lambda s: jnp.clip(s - n_mul, 0, n_mid - 1)
    out_at = lambda s: jnp.maximum(s - n_mul - n_mid, 0)
    full = lambda shape: pl.BlockSpec(shape, lambda s, q: (0,) * len(shape))
    part_spec = lambda arr: pl.BlockSpec((MID_CH,) + arr.shape[1:], lambda s, q: (mul_at(s), 0, 0))
    piece_spec = lambda n: pl.BlockSpec((MID_ROWS, half, chans), lambda s, q: (mid_at(s), q[n], 0))
    do_spec = pl.BlockSpec((MID_CH, half, rows), lambda s, q: (out_at(s), 0, 0))
    do_type = jax.ShapeDtypeStruct((chans, half, rows), BF16)
    mats = jax.ShapeDtypeStruct((chans, chans), F32)
    return pl.pallas_call(
        functools.partial(middle_kernel, n_mul, n_mid, len(b_parts)),
        grid_spec=pltpu.PrefetchScalarGridSpec(
            num_scalar_prefetch=1,
            grid=(2 * n_mul + n_mid,),
            in_specs=[
                pl.BlockSpec((MID_CH, rows, n_col), lambda s, q: (mul_at(s), 0, 0)),
                *[part_spec(arr) for arr in b_parts],
                piece_spec(0), piece_spec(1), piece_spec(0), piece_spec(1),
                full(wg_t.shape), full(wo.shape), full(wo_t.shape), full(scale.shape), full(offset.shape)]
            + [pl.BlockSpec(memory_space=pl.ANY)] * len(after),
            out_specs=[
                do_spec, do_spec,
                pl.BlockSpec((MID_ROWS, chans, LANES), lambda s, q: (mid_at(s), 0, 0)),
                full((chans, chans)), full((chans, chans)), full((4, chans, LANES))],
            scratch_shapes=[pltpu.VMEM((chans * (LANES + 1), LANES), F32)],
        ),
        out_shape=[
            do_type, do_type,
            jax.ShapeDtypeStruct((rows, chans, LANES), BF16),
            mats, mats, jax.ShapeDtypeStruct((4, chans, LANES), F32)],
        compiler_params=pltpu.CompilerParams(vmem_limit_bytes=VMEM_LIMIT),
        cost_estimate=pl.CostEstimate(flops=25 * 10 ** 9, bytes_accessed=48 * 2 ** 20, transcendentals=0),
        name='middle',
    )(pieces, act_a, *b_parts, zn, zn, dy_rows, dy_rows, wg_t, wo, wo_t, scale, offset, *after)


def grad_kernel(trans, n_do, n_act, n_seed, partial, *refs):
    grads, acts, rest = refs[:n_do], refs[n_do:n_do + n_act], refs[n_do + n_act:]
    step = acts[0].shape[0]
    pitch = step + 1

    def product(c):
        if trans:
            lhs = jnp.concatenate([g[c] for g in grads], axis=0)
        else:
            lhs = jnp.concatenate([jnp.concatenate([g[c] for g in grads[n:n + 2]], axis=1) for n in range(0, n_do, 2)], axis=0)
        rhs = jnp.concatenate([act[c] for act in acts], axis=0)
        acc = dot_tn(lhs, rhs) if trans else dot_nn(lhs, rhs)
        return acc + rest[0][c] if n_seed else acc

    if partial:
        out_ref = rest[-1]

        def block(n, carry):
            for j in range(4):
                out_ref[4 * n + j] = product(4 * n + j)
            return carry

        lax.fori_loop(0, step // 4, block, 0)
        return
    mask_ref, out_ref, scr = rest[n_seed], rest[-2], rest[-1]
    rows, n_col = mask_ref.shape
    plane = rows * pitch

    def block(n, carry):
        for j in range(4):
            acc = product(4 * n + j) * mask_ref[...]
            for t in range(n_col // LANES):
                scr[pl.ds(t * plane + 4 * n + j, rows, stride=pitch), :] = acc[:, t * LANES:(t + 1) * LANES]
        return carry

    lax.fori_loop(0, step // 4, block, 0)

    def pack(i, carry):
        for t in range(n_col // LANES):
            out_ref[i, :, t * LANES:(t + 1) * LANES] = scr[pl.ds(t * plane + i * pitch, step), :].astype(BF16)
        return carry

    lax.fori_loop(0, rows, pack, 0, unroll=8)


def grad_sum(trans, grads, acts, mask_f, part=0, parts=1, seed=None, partial=False, after=()):
    chans = grads[0].shape[0]
    n_col = acts[0].shape[2]
    rows = mask_f.shape[0] // parts
    step = MID_CH
    block = lambda arr: pl.BlockSpec((step,) + arr.shape[1:], lambda s: (s, 0, 0))
    sum_spec = lambda at: pl.BlockSpec((step, rows, n_col), lambda s: (s, at, 0))
    seeds = [] if seed is None else [seed]
    if partial:
        masks, scratch = [], []
        out_spec, out_shape = sum_spec(0), jax.ShapeDtypeStruct((chans, rows, n_col), F32)
    else:
        masks, scratch = [mask_f], [pltpu.VMEM((n_col // LANES * rows * (step + 1), LANES), F32)]
        out_spec = pl.BlockSpec((rows, step, n_col), lambda s: (0, s, 0))
        out_shape = jax.ShapeDtypeStruct((rows, chans, n_col), BF16)
    return pl.pallas_call(
        functools.partial(grad_kernel, trans, len(grads), len(acts), len(seeds), partial),
        grid=(chans // step,),
        in_specs=[block(arr) for arr in list(grads) + list(acts)] + [sum_spec(part)] * len(seeds)
        + [pl.BlockSpec((rows, n_col), lambda s: (part, 0))] * len(masks) + [pl.BlockSpec(memory_space=pl.ANY)] * len(after),
        out_specs=out_spec,
        out_shape=out_shape,
        scratch_shapes=scratch,
        compiler_params=pltpu.CompilerParams(vmem_limit_bytes=VMEM_LIMIT),
        cost_estimate=pl.CostEstimate(flops=12 * 10 ** 9, bytes_accessed=80 * 2 ** 20, transcendentals=0),
    )(*grads, *acts, *seeds, *masks, *after)


def final_kernel(seeded, q_ref, z_ref, dy_ref, da_ref, db_ref, gl0, gl1, gl2, gl3, w_ref, wb_ref, scale_ref, offset_ref, *refs):
    dz_ref, dw_ref, dbin_ref, vec_ref = refs[-4:]
    gls = (gl0, gl1, gl2, gl3)
    chans = z_ref.shape[2]
    n_lane = z_ref.shape[1] // LANES
    side = LANES // 2

    @pl.when(pl.program_id(0) == 0)
    def _():
        if seeded:
            for ref, seed in zip((dw_ref, dbin_ref, vec_ref), refs[:3]):
                ref[...] = seed[...]
        else:
            dw_ref[...] = jnp.zeros_like(dw_ref)
            dbin_ref[...] = jnp.zeros_like(dbin_ref)
            vec_ref[...] = jnp.zeros_like(vec_ref)

    one16 = ones_row(n_lane * LANES)

    def row(i, carry):
        qs = [q_ref[t] for t in range(n_lane)]
        offs = [pl.multiple_of(q * LANES, LANES) for q in qs]
        fold = lambda val: sum(val[:, t * LANES:(t + 1) * LANES] for t in range(n_lane))
        z_rows = jnp.concatenate([z_ref[i, pl.ds(off, LANES), :] for off in offs], axis=0)
        x_hat, inv_std, znt = input_norm(z_rows, scale_ref[...], offset_ref[...])
        proj = dot_nn(w_ref[...], jnp.concatenate([znt, one16], axis=0))
        grad16 = []
        for g in range(chans // GROUP):
            parts = [proj[(4 * g + n) * GROUP:(4 * g + n + 1) * GROUP] for n in range(4)]
            vals = [None] * 4
            for n, ref in enumerate((da_ref, db_ref)):
                grad = jnp.concatenate([ref[i, g * GROUP:(g + 1) * GROUP, pl.ds(off, LANES)] for off in offs], axis=1).astype(F32)
                sig = jax.nn.sigmoid(parts[2 + n])
                vals[n] = grad * sig
                vals[2 + n] = vals[n] * parts[n] * (1.0 - sig)
            for n in range(4):
                dbin_ref[(4 * g + n) * GROUP:(4 * g + n + 1) * GROUP] += fold(vals[n])
                grad16.append(vals[n].astype(BF16))
        grad16 = jnp.concatenate(grad16, axis=0)
        gate = [g[i] for g in gls[:2]] + [g[i][:, part] for part in (slice(0, side), slice(side, LANES)) for g in gls[2:]]
        gate = jnp.concatenate(gate, axis=1)
        dw_ref[...] += dot_nn(grad16, jnp.transpose(znt))
        d_znorm = dot_nn(wb_ref[...], jnp.concatenate([grad16, gate], axis=0)).astype(BF16).astype(F32)
        vec_ref[0] += fold(d_znorm * x_hat)
        vec_ref[1] += fold(d_znorm)
        grad_hat = d_znorm * scale_ref[...]
        d_in = inv_std * (grad_hat - col_mean(grad_hat) - x_hat * col_mean(grad_hat * x_hat))
        d_rows = jnp.transpose(d_in)
        for t in range(n_lane):
            out = d_rows[t * LANES:(t + 1) * LANES] + dy_ref[i, pl.ds(offs[t], LANES), :].astype(F32)
            dz_ref[i, pl.ds(offs[t], LANES), :] = out.astype(BF16)
        return carry

    lax.fori_loop(0, ROWS, row, 0, unroll=4)


def final(q_all, z_rows, dy_rows, d_a, d_b, gates, w_t, w_back, scale, offset, first, d_z=None, seeds=()):
    _, n_col, chans = z_rows.shape
    n_step = d_b.shape[0] // ROWS
    at = first // ROWS
    full = lambda shape: pl.BlockSpec(shape, lambda s, q: (0,) * len(shape))
    pair_spec = pl.BlockSpec((ROWS, n_col, chans), lambda s, q: (s + at, 0, 0))
    sums = [(4 * chans, chans), (4 * chans, LANES), (2, chans, LANES)]
    args = [q_all, z_rows, dy_rows, d_a, d_b, *gates, w_t, w_back, scale, offset, *seeds]
    in_specs = ([pair_spec, pair_spec, pl.BlockSpec((ROWS, chans, n_col), lambda s, q: (s + at, 0, 0)),
                 pl.BlockSpec((ROWS, chans, n_col), lambda s, q: (s, 0, 0))]
                + [pl.BlockSpec((ROWS, chans, LANES), lambda s, q: (s + at, 0, 0))] * 4
                + [full(w_t.shape), full(w_back.shape), full(scale.shape), full(offset.shape)]
                + [full(seed.shape) for seed in seeds])
    alias = {}
    if d_z is not None:
        alias = {len(args): 0}
        args.append(d_z)
        in_specs.append(pl.BlockSpec(memory_space=pl.ANY))
    return pl.pallas_call(
        functools.partial(final_kernel, bool(seeds)),
        grid_spec=pltpu.PrefetchScalarGridSpec(
            num_scalar_prefetch=1,
            grid=(n_step,),
            in_specs=in_specs,
            out_specs=[pair_spec] + [full(shape) for shape in sums],
        ),
        out_shape=[jax.ShapeDtypeStruct(z_rows.shape, BF16)] + [jax.ShapeDtypeStruct(shape, F32) for shape in sums],
        input_output_aliases=alias,
        compiler_params=pltpu.CompilerParams(vmem_limit_bytes=VMEM_LIMIT),
        cost_estimate=pl.CostEstimate(flops=30 * 10 ** 9, bytes_accessed=64 * 2 ** 20, transcendentals=0),
        name='final',
    )(*args)


def lane_bcast(vec, width):
    return jnp.broadcast_to(vec.astype(F32)[:, None], (vec.shape[0], width))


def local_step(z_loc, mask_loc, dy_loc, ln_in_scale, ln_in_offset, w_in, b_in, ln_out_scale, ln_out_offset, w_out, b_out, w_gate, b_gate):
    n_dap = lax.axis_size('dap')
    me = lax.axis_index('dap')
    swap = lambda arr, bit: lax.ppermute(arr, 'dap', [(d, d ^ bit) for d in range(n_dap)])
    w_t = with_bias(by_group(w_in).T, by_group(b_in))
    row_sc, row_of = (lane_bcast(v, z_loc.shape[1]) for v in (ln_in_scale, ln_in_offset))
    in_sc, in_of = lane_bcast(ln_in_scale, 256), lane_bcast(ln_in_offset, 256)
    out_sc, out_of = lane_bcast(ln_out_scale, 256), lane_bcast(ln_out_offset, 256)
    z_far = swap(z_loc, 2)
    rows = z_loc.shape[0]
    part = rows // 4
    mask_f = mask_loc.astype(F32)
    mask_loc = mask_loc.reshape(rows, -1, 1, LANES)
    mask_far = swap(mask_loc, 2)
    n_chunk = rows // part
    z_far = []
    for n in range(n_chunk):
        z_from = lax.optimization_barrier(z_loc) if n else z_loc
        z_far.append(swap(z_from[n * part:(n + 1) * part], 2))
    weights = (w_t, in_sc, in_of)
    a_0, b_0, zn = project(z_loc, mask_loc, 0, rows, *weights, True)
    b_1 = swap(b_0, 1)
    a_1 = swap(a_0, 1)
    blocks = [me ^ r for r in range(n_dap)]
    tail = (zn, dy_loc, with_bias(w_gate.T, b_gate), w_out, with_bias(w_out.T, b_out), out_sc, out_of)
    pieces = lambda *vals: jnp.stack(vals).astype(jnp.int32)
    mids = [middle(pieces(2 * blocks[0], 2 * blocks[0] + 1), a_0, [b_0], *tail)]
    mids.append(middle(pieces(2 * blocks[1], 2 * blocks[1] + 1), a_0, [b_1], *tail, after=(mids[0][5],)))
    near_out = [swap(mids[1][0], 1), swap(mids[1][1], 1)]
    a_2, b_2, a_3, b_3, far_out = [], [], [], [], []
    far_b = lambda h: b_2[2 * h:2 * h + 2] + b_3[2 * h:2 * h + 2]
    d_outs = lambda *tiles: [mids[t][n] for t in tiles for n in range(2)]
    order = (mids[1][5],)
    for h in range(2):
        for n in (2 * h, 2 * h + 1):
            a_n, b_n = project(z_far[n], mask_far, n * part, part, *weights, False, after=order)
            b_3.append(swap(b_n, 1))
            a_3.append(swap(a_n, 1))
            a_2.append(a_n)
            b_2.append(b_n)
            order = (a_n,)
            if n == 1:
                part_b = grad_sum(False, [mids[0][0], near_out[0], mids[0][1], near_out[1]], [a_0, a_1], mask_f, partial=True, after=order)
                order = (part_b,)
            if n == 2:
                part_a = grad_sum(True, d_outs(0, 1, 2), [b_0, b_1, *far_b(0)], mask_f, partial=True, after=order)
                order = (part_a,)
        mids.append(middle(pieces(2 * blocks[2] + h, 2 * blocks[3] + h), a_0, far_b(h), *tail, after=order))
        order = (mids[-1][5],)
        far_out.append([swap(mids[2 + h][0], 2), swap(mids[2 + h][1], 3)])
    d_a = grad_sum(True, d_outs(3), far_b(1), mask_f, seed=part_a)
    w_back = jnp.concatenate([by_group(w_in), w_gate], axis=1)
    d_z, seeds = None, ()
    for h in range(2):
        d_b = grad_sum(False, far_out[h], [*a_2, *a_3], mask_f, part=h, parts=2, seed=part_b, after=(d_a,) if h == 0 else (seeds[2],))
        d_z, *seeds = final(jnp.stack(blocks).astype(jnp.int32), z_loc, dy_loc, d_a, d_b, [m[2] for m in mids], w_t, w_back, row_sc, row_of,
                            h * (rows // 2), d_z, seeds)
    dw_t, dbin, vecs = seeds
    d_wo = sum(m[3] for m in mids)
    d_wg = sum(m[4] for m in mids).T
    vec_mid = jnp.sum(sum(m[5] for m in mids), axis=-1)
    vec_in = jnp.sum(vecs, axis=-1)
    summed = lax.psum((vec_in[0], vec_in[1], dw_t, jnp.sum(dbin, axis=-1), vec_mid[0], vec_mid[1], d_wo, vec_mid[2], d_wg, vec_mid[3]), 'dap')
    summed = list(summed)
    summed[2] = from_group(summed[2].T)
    summed[3] = from_group(summed[3])
    return (d_z,) + tuple(piece.astype(BF16) for piece in summed)


def solution(mesh):
    pair_spec = P(('batch', 'dap'), None, None)
    mask_spec = P(('batch', 'dap'), None)
    vec_rep = P(None)
    mat_rep = P(None, None)
    vec_part = P('batch')
    mat_part = P('batch', None)
    in_specs = (pair_spec, mask_spec, pair_spec, vec_rep, vec_rep, mat_rep, vec_rep, vec_rep, vec_rep, mat_rep, vec_rep, mat_rep, vec_rep)
    out_specs = (pair_spec, vec_part, vec_part, mat_part, vec_part, vec_part, vec_part, mat_part, vec_part, mat_part, vec_part)
    return jax.shard_map(local_step, mesh=mesh, in_specs=in_specs, out_specs=out_specs, check_vma=False)
```
